32 devices in a mesh: scene: 4 (over y, core), tile: 8 (over z, x).
Axes of the slice: x: 2, y: 2, z: 4, core: 2. Of those that a mesh axis runs over, the one named last changes fastest.
Arguments:
- node_latent: bfloat16 [131072, 128], P(('scene', 'tile')), parts along dimension 0, may hold values from -6 to 6
- cotangent: float32 [131072, 128], P(('scene', 'tile')), parts along dimension 0, may hold values from -6 to 6
- neighbours: int32 [12, 131072], P(None, ('scene', 'tile')), parts along dimension 1, may hold values from -1 to 6143, as said below
- send_rows: int32 [32, 2, 1024], P(('scene', 'tile')), parts along dimension 0, may hold values from 0 to 4095
- node_mask: int32 [131072], P(('scene', 'tile')), parts along dimension 0, may hold values 0 or 1
- w_src: bfloat16 [128, 128], replicated, may hold values from -0.5 to 0.5
- w_dst: bfloat16 [128, 128], replicated, may hold values from -0.5 to 0.5
- w_msg: bfloat16 [128, 128], replicated, may hold values from -0.5 to 0.5
- edge_gain: float32 [128], replicated, may hold values from 0.1 to 1.9
- edge_bias: float32 [128], replicated, may hold values from -3 to 3
- w_self: bfloat16 [128, 128], replicated, may hold values from -0.5 to 0.5
- w_agg: bfloat16 [128, 128], replicated, may hold values from -0.5 to 0.5
- node_bias: float32 [128], replicated, may hold values from -3 to 3
- w_out: bfloat16 [128, 128], replicated, may hold values from -0.5 to 0.5
Outputs:
- updated: bfloat16 [131072, 128], P(('scene', 'tile')), parts along dimension 0
- latent_grad: float32 [131072, 128], P(('scene', 'tile')), parts along dimension 0
- grad_src: float32 [512, 128], P('scene'), parts along dimension 0
- grad_dst: float32 [512, 128], P('scene'), parts along dimension 0
- grad_msg: float32 [512, 128], P('scene'), parts along dimension 0
- grad_edge_gain: float32 [512], P('scene'), parts along dimension 0
- grad_edge_bias: float32 [512], P('scene'), parts along dimension 0
- grad_self: float32 [512, 128], P('scene'), parts along dimension 0
- grad_agg: float32 [512, 128], P('scene'), parts along dimension 0
- grad_node_bias: float32 [512], P('scene'), parts along dimension 0
- grad_out: float32 [512, 128], P('scene'), parts along dimension 0
The draws below stay inside these ranges and needn't reach their ends.
There are 4 independent parts, one for each index of `scene`. The reference program is written for one: setup_inputs(seed, part) draws one part's arguments, and reference() takes and returns one part's arrays. A program takes and returns all parts, laid end to end along the dimension named above; an argument that names none is the same for every part. Nothing has to cross between parts.
Inputs may be any that keep to these rules, and one draw needn't show every extreme that they name: `neighbours`: each entry is -1 (empty slot) or a row of the tile's extended list: below 4096 its own nodes, then 1024 rows from the tile below, then 1024 rows from the tile above. `send_rows`: rows of the sending tile's own nodes; a row may appear more than once.
All inputs are finite; a program needn't handle non-finite values. No bound on the sum of `node_mask` on one device may be relied on, other than what follows from the above.
Results may differ from the reference program's by a relative error of at most 0.028.
Values may be sent and summed in bfloat16 or wider, within the bound.
A program may use at most 448 MiB of HBM per device.

```python
from functools import partial
import jax
import jax.numpy as jnp
from jax import lax

W = 128
DEG = 12
NDEV = 4096
HALO = 1024
TILES = 8
NODES = 32768
N_TILE = 8


def draw_neighbours(key, part):
    shape = (DEG, NODES)
    kinds = jax.random.randint(jax.random.fold_in(key, 11), shape, 0, 20)
    owned = jax.random.randint(jax.random.fold_in(key, 12), shape, 0, NDEV)
    remote = jax.random.randint(jax.random.fold_in(key, 13), shape, NDEV, NDEV + 2 * HALO)
    return jnp.where(kinds < 2, -1, jnp.where(kinds < 5, remote, owned)).astype(jnp.int32)


def set_ends(array, key, low, high):
    index_at = [jax.random.randint(jax.random.fold_in(key, axis), (), 0, length) for axis, length in enumerate(array.shape)]
    longest = array.shape.index(max(array.shape))
    beside = index_at[:longest] + [(index_at[longest] + 1) % array.shape[longest]] + index_at[longest + 1:]
    return array.at[tuple(index_at)].set(low).at[tuple(beside)].set(high)


def level_of(key, extent, cuts, smallest, top_value):
    def one(dim, parts):
        steps = jax.random.uniform(jax.random.fold_in(jax.random.fold_in(key, 6), dim), (parts,), jnp.float32, smallest / len(cuts), top_value / len(cuts))
        return jnp.repeat(jnp.exp(steps), extent[dim] // parts).reshape((-1,) + (1,) * (len(extent) - dim - 1))

    level = one(*cuts[0])
    for cut in cuts[1:]:
        level = level * one(*cut)
    return level


def gaussian(own_key, shape, deviation, bound, split=(), dtype=jnp.bfloat16):
    entries = jax.random.normal(own_key, shape, jnp.float32) * deviation
    if len(split) > 0:
        entries = level_of(own_key, shape, split, -0.22, 0.18) * entries
    return jnp.clip(entries, min=-bound, max=bound).astype(dtype)


def setup_inputs(seed: int = 0, part: int = 0) -> dict:
    streams_of = jax.random.split(jax.random.key(seed), 15)
    part_keys = jax.random.split(jax.random.fold_in(streams_of[14], part), 15)
    node_latent = gaussian(part_keys[0], (NODES, W), 1.0, 6.0, ((0, 8),))
    cotangent = gaussian(part_keys[1], (NODES, W), 1.0, 6.0, ((0, 8),), jnp.float32)
    neighbours = draw_neighbours(jax.random.fold_in(jax.random.fold_in(streams_of[14], part), 71), part)
    send_rows = set_ends(jax.random.randint(part_keys[3], (TILES, 2, HALO), 0, NDEV), jax.random.fold_in(part_keys[3], 1), 0, NDEV - 1).astype(jnp.int32)
    node_mask = set_ends((jax.random.randint(part_keys[4], (NODES,), 0, 4) < 3).astype(jnp.int32), jax.random.fold_in(part_keys[4], 1), 0, 1)
    w_src = gaussian(streams_of[5], (W, W), W ** -0.5, 0.5)
    w_dst = gaussian(streams_of[6], (W, W), W ** -0.5, 0.5)
    w_msg = gaussian(streams_of[7], (W, W), W ** -0.5, 0.5)
    edge_gain = jnp.clip(1.0 + 0.18 * jax.random.normal(streams_of[8], (W,), jnp.float32), 0.1, 1.9)
    edge_bias = gaussian(streams_of[9], (W,), 0.5, 3.0, (), jnp.float32)
    w_self = gaussian(streams_of[10], (W, W), W ** -0.5, 0.5)
    w_agg = gaussian(streams_of[11], (W, W), W ** -0.5, 0.5)
    node_bias = gaussian(streams_of[12], (W,), 0.5, 3.0, (), jnp.float32)
    w_out = gaussian(streams_of[13], (W, W), W ** -0.5, 0.5)
    return dict(node_latent=node_latent, cotangent=cotangent, neighbours=neighbours, send_rows=send_rows, node_mask=node_mask, w_src=w_src, w_dst=w_dst, w_msg=w_msg, edge_gain=edge_gain, edge_bias=edge_bias, w_self=w_self, w_agg=w_agg, node_bias=node_bias, w_out=w_out)


def edge_block(w_msg, edge_gain, proj_src, pieces):
    source, proj_part = pieces
    present = (source >= 0)[:, :, None]
    gathered = proj_src[jnp.maximum(source, 0)] + proj_part[None]
    hidden = jax.nn.silu(gathered).astype(jnp.bfloat16)
    degree, block_rows, feature = hidden.shape
    message = jnp.dot(hidden.reshape(degree * block_rows, feature), w_msg.astype(jnp.bfloat16), preferred_element_type=jnp.float32)
    message = message.reshape(degree, block_rows, feature)
    centre = lax.optimization_barrier(jnp.mean(message, axis=2, keepdims=True))
    spread = lax.optimization_barrier(jnp.mean(jnp.square(message - centre), axis=2, keepdims=True))
    normed = (message - centre) * lax.rsqrt(spread + 1e-05) * edge_gain
    return lax.optimization_barrier(jnp.sum(jnp.where(present, normed, 0.0), axis=0))

def edge_section(eparams, extended32, neighbours, again):
    w_src, w_dst, w_msg, edge_gain, edge_bias = eparams
    degree, node_count = neighbours.shape
    extended = extended32.astype(jnp.bfloat16)
    proj_src = jnp.dot(extended, w_src.astype(jnp.bfloat16), preferred_element_type=jnp.float32)
    proj_dst = jnp.dot(extended[:node_count], w_dst.astype(jnp.bfloat16), preferred_element_type=jnp.float32) + edge_bias
    block_rows = min(node_count, 1024)
    nblocks = node_count // block_rows
    groups = neighbours.reshape(degree, nblocks, block_rows).transpose(1, 0, 2)
    worker = partial(edge_block, w_msg, edge_gain, proj_src)
    if again:
        worker = jax.checkpoint(worker)
    summed = lax.map(worker, (groups, proj_dst.reshape(nblocks, block_rows, -1)))
    return summed.reshape(node_count, -1)

def node_section(nparams, own32, summed_bf, node_mask):
    w_self, w_agg, node_bias, w_out = nparams
    own = own32.astype(jnp.bfloat16)
    inner = jnp.dot(own, w_self.astype(jnp.bfloat16), preferred_element_type=jnp.float32)
    inner = inner + jnp.dot(summed_bf, w_agg.astype(jnp.bfloat16), preferred_element_type=jnp.float32) + node_bias
    update = jax.nn.silu(inner).astype(jnp.bfloat16)
    return own32 + node_mask.astype(jnp.float32)[:, None] * jnp.dot(update, w_out.astype(jnp.bfloat16), preferred_element_type=jnp.float32)

def tile_forward(params, extended32, neighbours, node_mask):
    node_count = neighbours.shape[1]
    summed = edge_section(params[:5], extended32, neighbours, False)
    return node_section(params[5:], extended32[:node_count], summed.astype(jnp.bfloat16), node_mask)

def reference(node_latent, cotangent, neighbours, send_rows, node_mask, w_src, w_dst, w_msg, edge_gain, edge_bias, w_self, w_agg, node_bias, w_out):
    params = tuple((p.astype(jnp.float32) for p in (w_src, w_dst, w_msg, edge_gain, edge_bias, w_self, w_agg, node_bias, w_out)))
    latent32 = node_latent.astype(jnp.float32)
    tiled_nbr = neighbours.reshape(DEG, N_TILE, NDEV).transpose(1, 0, 2)
    tiled_mask = node_mask.reshape(N_TILE, NDEV)

    def scene(params, latent32):
        tiled = latent32.reshape(N_TILE, NDEV, W)
        down_send = jax.vmap(lambda block, listing: block[listing])(tiled, send_rows[:, 0])
        up_send = jax.vmap(lambda block, listing: block[listing])(tiled, send_rows[:, 1])
        extended = jnp.concatenate([tiled, jnp.roll(up_send, 1, axis=0), jnp.roll(down_send, -1, axis=0)], axis=1)

        def one_tile(pieces):
            return tile_forward(params, pieces[0], pieces[1], pieces[2])
        result = lax.map(jax.checkpoint(one_tile), (extended, tiled_nbr, tiled_mask))
        return result.reshape(NODES, W)
    result, backward = jax.vjp(scene, params, latent32)
    grads, latent_grad = backward(cotangent)
    factor = NODES ** (-0.5)
    grads = tuple((g * factor for g in grads))
    return (result.astype(jnp.bfloat16), latent_grad, grads[0], grads[1], grads[2], grads[3], grads[4], grads[5], grads[6], grads[7], grads[8])
```

```python
import functools

import jax
import jax.numpy as jnp
from jax import lax
from jax.experimental import pallas as pl
from jax.experimental.pallas import tpu as pltpu
from jax.sharding import PartitionSpec as P

CHUNK = 32
RING = 9
COPIES = 8
EMPTY = -1e4
PLAN = (
    "c1", ("s", 1), ("g", 1), "c2", ("s", 2), ("g", 2), "d1", ("s", 3), ("g", 3), "e1", ("s", 4), ("g", 4), "n2", ("s", 5), ("g", 5), "n1", ("s", 6), ("g", 6), "f1", ("s", 7), ("g", 7), ("s", 8), ("g", 8), "p1", ("s", 9), ("g", 9), "c1s", ("s", 10), ("g", 10), "d2", ("s", 11), ("g", 11), "e2", ("s", 12), ("g", 12), "n3", ("s", 13), ("g", 13), "n4", ("s", 14), ("g", 14), "n1s", ("s", 15), ("g", 15), "n5", ("s", 16), ("g", 16), ("s", 17), ("g", 17), "c3", ("s", 18), ("g", 18), "e3", ("s", 19), ("g", 19), ("s", 20), ("g", 20), "e3", ("s", 21), ("g", 21), ("s", 22), ("g", 22), "e3", ("s", 23), ("g", 23), ("s", 24), ("g", 24),
)
BF = jnp.bfloat16
F32 = jnp.float32


def mm(a, b):
    return jnp.dot(a, b, preferred_element_type=F32)


def mm_nt(a, b):
    return lax.dot_general(a, b, (((1,), (1,)), ((), ())), preferred_element_type=F32)


def mm_tn(a, b):
    return lax.dot_general(a, b, (((0,), (0,)), ((), ())), preferred_element_type=F32)


def sigmoid(x):
    return 0.5 * jnp.tanh(0.5 * x) + 0.5


def layer_kernel(
    degree,
    chunk,
    idx_ref,
    ct_ref,
    live_ref,
    ext_ref,
    w_src_ref,
    w_half_ref,
    w_dst_ref,
    w_back_ref,
    w_cent_ref,
    gain_ref,
    ebias_ref,
    w_self_ref,
    w_agg_ref,
    nbias_ref,
    w_out_ref,
    updated_ref,
    down_ref,
    halo_ref,
    gw_ref,
    gv_ref,
    table,
    hid,
    slope,
    yhat,
    rstd,
    dmsg,
    dhid,
    ysums,
    dycs,
    bases,
    sums,
    hid_new,
    slope_new,
    dps,
    pds,
    cents,
    pres,
    dinners,
    sbs,
    dobs,
    *accs,
):
    nodes, width = down_ref.shape
    listed = ext_ref.shape[0]
    copies = len(accs)
    steps = nodes // chunk
    edges = degree * chunk
    half = edges // 2
    groups = edges // 8

    table[pl.ds(0, listed), :] = mm(ext_ref[...], w_half_ref[...])
    table[pl.ds(listed, 8), :] = jnp.full((8, width), EMPTY, F32)
    for ref in (
        slope, yhat, rstd, dmsg, dhid, ysums, dycs, sums, hid, hid_new, slope_new, dps,
        cents, pres, dinners, sbs, dobs, *accs,
    ):
        ref[...] = jnp.zeros_like(ref)
    gw_ref[...] = jnp.zeros_like(gw_ref)

    ones = jnp.full((width, width), 1.0 / width, BF)
    zeros = jnp.zeros((width, width), BF)
    ones2 = jnp.concatenate(
        [jnp.concatenate([ones, zeros], 1), jnp.concatenate([zeros, ones], 1)], 0
    )
    at_row = lax.broadcasted_iota(jnp.int32, (8, width), 0)
    bit = [(at_row & b) != 0 for b in (1, 2, 4)]
    only = [at_row == j for j in range(8)]

    def rows_of(m):
        return pl.ds(pl.multiple_of(jnp.clip(m, 0, steps - 1) * chunk, chunk), chunk)

    def list_of(m):
        at = jnp.clip(m, 0, steps - 1)
        return lambda e: idx_ref.at[pl.ds(e * steps, steps)][at]

    def body(m, carry):
        gain = gain_ref[...]

        def slot(lag):
            return lax.rem(m + 2 * RING - lag, RING)

        v = {"pd": pds[...]}
        per = chunk // 8
        dpd = [None] * per
        idx0 = list_of(m)
        idx7 = list_of(m - 7)
        s7 = slot(7)

        def wide(x):
            return jnp.concatenate([x[:half], x[half:]], 1)

        def fold(x):
            return sum(x[i * 8 : i * 8 + 8] for i in range(1, per)) + x[:8]

        def gather(g):
            rows = [
                jnp.broadcast_to(table[pl.ds(idx0(g * 8 + j), 1), :], (8, width))
                for j in range(8)
            ]
            for b in bit:
                rows = [jnp.where(b, q, p) for p, q in zip(rows[::2], rows[1::2])]
            n = g % per
            z = rows[0] + v["pd"][n * 8 : n * 8 + 8]
            t = jnp.tanh(z)
            q = 1.0 + t
            h = z * q
            slope_new[pl.ds(g * 8, 8), :] = q + h * (1.0 - t)
            return h

        def scatter(chunks):
            for g in chunks:
                at = pl.ds(g * 8, 8)
                dx = dhid[at, :] * slope[s7, at, :]
                n = g % per
                dpd[n] = dx if dpd[n] is None else dpd[n] + dx
                for j in range(8):
                    acc = accs[(g * 8 + j) % copies]
                    to = pl.ds(idx7(g * 8 + j) + (8 - j), 8)
                    pltpu.store(acc.at[to, :], acc[to, :] + dx, mask=only[j])

        def c1():
            old = hid_new[...]
            hid[slot(1)] = old
            slope[slot(1)] = slope_new[...]
            v["c"] = mm(wide(old), w_cent_ref[...])

        def c1s():
            cents[...] = v["c"]

        def c2():
            v["c2"] = cents[...]
            v["var"] = mm((v["c2"] * v["c2"]).astype(BF), ones2)

        def c3():
            r = lax.rsqrt(v["var"] + 1e-5)
            y = v["c2"] * r
            yhat[slot(2)] = y
            rstd[slot(2)] = r
            ys = y[:, :width] + y[:, width:]
            ysums[slot(2)] = (
                sum(ys[i * chunk : (i + 1) * chunk] for i in range(1, degree // 2))
                + ys[:chunk]
            )

        def n1():
            at = rows_of(m - 3)
            own = ext_ref[at, :]
            sb = (ysums[slot(3)] * gain).astype(BF)
            v["pre"] = (
                mm(own, w_self_ref[...]) + mm(sb, w_agg_ref[...]) + nbias_ref[...]
            )
            inside = jnp.logical_and(m >= 3, m < steps + 3).astype(F32)
            dob = (inside * live_ref[at, :].astype(F32) * ct_ref[at, :]).astype(BF)
            v["dinner"] = mm_nt(dob, w_out_ref[...])
            v["sb"] = sb
            v["dob"] = dob

        def n1s():
            pres[...] = v["pre"]
            dinners[...] = v["dinner"]
            sbs[...] = v["sb"]
            dobs[...] = v["dob"]

        def n2():
            pre = pres[...]
            sg = sigmoid(pre)
            u = pre * sg
            v["ub"] = u.astype(BF)
            v["dpre"] = dinners[...] * (sg + u - u * sg)
            v["dpb"] = v["dpre"].astype(BF)
            v["dsum"] = mm_nt(v["dpb"], w_agg_ref[...])

        def n3():
            at = rows_of(m - 4)
            own = ext_ref[at, :]
            updated_ref[at, :] = (
                own.astype(F32)
                + live_ref[at, :].astype(F32) * mm(v["ub"], w_out_ref[...])
            ).astype(BF)
            bases[slot(4)] = ct_ref[at, :] + mm_nt(v["dpb"], w_self_ref[...])
            sums[2] += fold(v["dpre"])

        def n4():
            gw_ref[3] += mm_tn(ext_ref[rows_of(m - 4), :], v["dpb"])
            gw_ref[4] += mm_tn(sbs[...], v["dpb"])
            gw_ref[5] += mm_tn(v["ub"], dobs[...])

        def n5():
            dy = v["dsum"] * gain
            dycs[...] = dy - jnp.mean(dy, axis=1, keepdims=True)
            sums[0] += fold(v["dsum"] * ysums[slot(4)])

        def d1():
            d = dycs[...]
            d = jnp.concatenate([d] * (degree // 2), 0)
            v["d"] = jnp.concatenate([d, d], 1)
            v["t"] = mm((v["d"] * yhat[slot(5)]).astype(BF), ones2)

        def d2():
            y = yhat[slot(5)]
            dm = (rstd[slot(5)] * (v["d"] - y * v["t"])).astype(BF)
            dmsg[pl.ds(0, half), :] = dm[:, :width]
            dmsg[pl.ds(half, half), :] = dm[:, width:]

        def e1():
            v["dm"] = dmsg[...]
            v["dh"] = mm(wide(v["dm"]), w_back_ref[...])

        def e2():
            gw_ref[2] += mm_tn(hid[slot(6)], v["dm"])

        def e3(first, last):
            for g in range(first, last):
                if g * 8 < half:
                    part = v["dh"][g * 8 : g * 8 + 8, :width]
                else:
                    part = v["dh"][g * 8 - half : g * 8 - half + 8, width:]
                dhid[pl.ds(g * 8, 8), :] = part

        def f1():
            at = rows_of(m - 8)
            dp = dps[...]
            dpdb = dp.astype(BF)
            down_ref[at, :] = bases[slot(8)] + mm_nt(dpdb, w_dst_ref[...])
            gw_ref[1] += mm_tn(ext_ref[at, :], dpdb)
            sums[1] += fold(dp)

        def p1():
            own = ext_ref[rows_of(m + 1), :]
            pds[...] = 0.5 * (mm(own, w_dst_ref[...]) + ebias_ref[...])

        stages = dict(
            c1=c1, c1s=c1s, c2=c2, c3=c3, n1=n1, n1s=n1s, n2=n2, n3=n3, n4=n4, n5=n5,
            d1=d1, d2=d2, e1=e1, e2=e2, f1=f1, p1=p1,
        )
        done = written = taken = 0
        for item in PLAN:
            if item == "e3":
                e3(written, done)
                written = done
            elif isinstance(item, str):
                stages[item]()
            else:
                kind, last = item[0], groups * item[1] // 24
                if kind == "s":
                    scatter(range(done, last))
                    done = last
                else:
                    for g in range(taken, last, 2):
                        pair = jnp.concatenate([gather(g), gather(g + 1)], 0)
                        hid_new[pl.ds(g * 8, 16), :] = pair.astype(BF)
                    taken = last
        e3(written, groups)
        dps[...] = jnp.concatenate(dpd, 0)
        return carry

    pds[...] = 0.5 * (mm(ext_ref[pl.ds(0, chunk), :], w_dst_ref[...]) + ebias_ref[...])
    lax.fori_loop(0, steps + 8, body, 0)

    gv_ref[...] = jnp.concatenate(
        [jnp.sum(sums[i], axis=0, keepdims=True) for i in range(3)]
        + [jnp.zeros((5, width), F32)],
        0,
    )
    dproj = accs[0][pl.ds(8, listed), :]
    for acc in accs[1:]:
        dproj = dproj + acc[pl.ds(8, listed), :]
    dpb = dproj.astype(BF)
    dext = mm_nt(dpb, w_src_ref[...])
    down_ref[...] += dext[:nodes]
    halo_ref[...] = dext[nodes:].astype(BF)
    gw_ref[0] = mm_tn(ext_ref[...], dpb)


def diagonal(w):
    zero = jnp.zeros_like(w)
    return jnp.concatenate(
        [jnp.concatenate([w, zero], 1), jnp.concatenate([zero, w], 1)], 0
    )


def layer(extended, cotangent, neighbours, node_mask, weights):
    w_src, w_dst, w_msg, edge_gain, edge_bias, w_self, w_agg, node_bias, w_out = weights
    degree, nodes = neighbours.shape
    width = cotangent.shape[1]
    listed = extended.shape[0]
    chunk = min(CHUNK, nodes)
    steps = nodes // chunk
    edges = degree * chunk
    idx = jnp.where(neighbours < 0, listed, neighbours)
    idx = idx.reshape(degree, steps, chunk).transpose(0, 2, 1).reshape(-1)
    live = jnp.broadcast_to(node_mask.astype(BF)[:, None], (nodes, width))
    w32 = w_msg.astype(F32)
    w_cent = (w32 - jnp.mean(w32, axis=1, keepdims=True)).astype(BF)
    half = jnp.asarray(0.5, BF)
    vmem = pl.BlockSpec(memory_space=pltpu.VMEM)
    return pl.pallas_call(
        functools.partial(layer_kernel, degree, chunk),
        in_specs=[pl.BlockSpec(memory_space=pltpu.SMEM)] + [vmem] * 14,
        out_specs=[vmem] * 5,
        out_shape=[
            jax.ShapeDtypeStruct((nodes, width), BF),
            jax.ShapeDtypeStruct((nodes, width), F32),
            jax.ShapeDtypeStruct((listed - nodes, width), BF),
            jax.ShapeDtypeStruct((6, width, width), F32),
            jax.ShapeDtypeStruct((8, width), F32),
        ],
        scratch_shapes=[
            pltpu.VMEM((listed + 8, width), F32),
            pltpu.VMEM((RING, edges, width), BF),
            pltpu.VMEM((RING, edges, width), F32),
            pltpu.VMEM((RING, edges // 2, 2 * width), F32),
            pltpu.VMEM((RING, edges // 2, 2 * width), F32),
            pltpu.VMEM((edges, width), BF),
            pltpu.VMEM((edges, width), F32),
            pltpu.VMEM((RING, chunk, width), F32),
            pltpu.VMEM((chunk, width), F32),
            pltpu.VMEM((RING, chunk, width), F32),
            pltpu.VMEM((3, 8, width), F32),
            pltpu.VMEM((edges, width), BF),
            pltpu.VMEM((edges, width), F32),
            pltpu.VMEM((chunk, width), F32),
            pltpu.VMEM((chunk, width), F32),
            pltpu.VMEM((edges // 2, 2 * width), F32),
            pltpu.VMEM((chunk, width), F32),
            pltpu.VMEM((chunk, width), F32),
            pltpu.VMEM((chunk, width), BF),
            pltpu.VMEM((chunk, width), BF),
        ]
        + [pltpu.VMEM((listed + 24, width), F32)] * COPIES,
        compiler_params=pltpu.CompilerParams(vmem_limit_bytes=60 * 2**20),
        name="layer",
    )(
        idx,
        cotangent,
        live,
        extended,
        w_src,
        w_src * half,
        w_dst,
        diagonal(w_msg.T * half),
        diagonal(w_cent),
        edge_gain[None],
        edge_bias[None],
        w_self,
        w_agg,
        node_bias[None],
        w_out,
    )


def finish_kernel(list_ref, back_ref, down_ref, out_ref):
    count = out_ref.shape[0]
    first = pl.program_id(0) * count
    span = list_ref.shape[1]
    here = lax.broadcasted_iota(jnp.int32, (count, span), 0) + first
    hit = jnp.where(here == list_ref[...], 1.0, 0.0).astype(BF)
    out_ref[...] = down_ref[...] + mm(hit, back_ref[...])


def finish(listing, back, down):
    nodes, width = down.shape
    count = min(512, nodes)
    rowed = pl.BlockSpec((count, width), lambda i: (i, 0))
    return pl.pallas_call(
        finish_kernel,
        grid=(nodes // count,),
        in_specs=[
            pl.BlockSpec((1, listing.shape[1]), lambda i: (0, 0)),
            pl.BlockSpec(back.shape, lambda i: (0, 0)),
            rowed,
        ],
        out_specs=rowed,
        out_shape=jax.ShapeDtypeStruct((nodes, width), F32),
        compiler_params=pltpu.CompilerParams(
            dimension_semantics=("arbitrary",), vmem_limit_bytes=60 * 2**20
        ),
        name="finish",
    )(listing, back, down)


def total_over(value, axis):
    size = lax.axis_size(axis)
    if size & (size - 1):
        return lax.psum(value, axis)
    bit = 1
    while bit < size:
        other = lax.ppermute(value, axis, [(i, i ^ bit) for i in range(size)])
        value = (value.astype(F32) + other.astype(F32)).astype(BF)
        bit *= 2
    return value


def on_device(node_latent, cotangent, neighbours, send_rows, node_mask, *weights):
    nodes = node_latent.shape[0]
    rim = send_rows.shape[2]
    size = lax.axis_size("tile")
    up = [(i, (i + 1) % size) for i in range(size)]
    down = [(j, i) for i, j in up]
    listing = send_rows.reshape(1, 2 * rim)
    outbound = node_latent[listing[0]]
    before = lax.ppermute(outbound[rim:], "tile", up)
    after = lax.ppermute(outbound[:rim], "tile", down)
    extended = jnp.concatenate([node_latent, before, after], axis=0)
    updated, down_grad, halo, gw, gv = layer(
        extended, cotangent, neighbours, node_mask, weights
    )
    to_below = lax.ppermute(halo[:rim], "tile", down)
    to_above = lax.ppermute(halo[rim:], "tile", up)
    back = jnp.concatenate([to_above, to_below], axis=0)
    packed = jnp.concatenate([gw.reshape(-1, gw.shape[2]), gv], axis=0).astype(BF)
    packed = total_over(packed, "tile").astype(F32)
    latent_grad = finish(listing, back, down_grad)
    packed = packed * (nodes * size) ** (-0.5)
    width = gw.shape[2]
    mats = [packed[i * width : (i + 1) * width] for i in range(6)]
    vecs = [packed[6 * width + i] for i in range(3)]
    return (
        updated,
        latent_grad,
        mats[0],
        mats[1],
        mats[2],
        vecs[0],
        vecs[1],
        mats[3],
        mats[4],
        vecs[2],
        mats[5],
    )


def solution(mesh):
    rowed, shared = P(("scene", "tile"), None), P()
    in_specs = (
        rowed,
        rowed,
        P(None, ("scene", "tile")),
        P(("scene", "tile"), None, None),
        P(("scene", "tile")),
    ) + (shared,) * 9
    mat, vec = P("scene", None), P("scene")
    out_specs = (rowed, rowed, mat, mat, mat, vec, vec, mat, mat, vec, mat)
    return jax.shard_map(
        on_device, mesh=mesh, in_specs=in_specs, out_specs=out_specs, check_vma=False
    )
```

```python
import functools

import jax
import jax.numpy as jnp
from jax import lax
from jax.experimental import pallas as pl
from jax.experimental.pallas import tpu as pltpu
from jax.sharding import PartitionSpec as P

CHUNK = 32
RING = 8
COPIES = 8
EMPTY = -1e4
PLAN = (
    "c1", "c2", ("s", 1), ("g", 1), "d1", "e1", ("s", 2), ("g", 2), "n2", "n1", ("s", 3), ("g", 3), "f1", "p1", ("s", 4), ("g", 4), ("s", 5), ("g", 5), "c1s", ("s", 6), ("g", 6), ("s", 7), ("g", 7), "d2", ("s", 8), ("g", 8), "e2", ("s", 9), ("g", 9), "n3", ("s", 10), ("g", 10), "n4", ("s", 11), ("g", 11), "n1s", ("s", 12), ("g", 12), "n5", ("s", 13), ("g", 13), "c3", ("s", 14), ("g", 14), "e3", ("s", 15), ("g", 15), ("s", 16), ("g", 16), "e3", ("s", 17), ("g", 17), ("s", 18), ("g", 18), ("s", 19), ("g", 19), ("s", 20), ("g", 20), ("s", 21), ("g", 21), ("s", 22), ("g", 22), ("s", 23), ("g", 23), "e3", ("s", 24), ("g", 24),
)
BF = jnp.bfloat16
F32 = jnp.float32
MESH = pl.DeviceIdType.MESH


def mm(a, b):
    return jnp.dot(a, b, preferred_element_type=F32)


def mm_nt(a, b):
    return lax.dot_general(a, b, (((1,), (1,)), ((), ())), preferred_element_type=F32)


def mm_tn(a, b):
    return lax.dot_general(a, b, (((0,), (0,)), ((), ())), preferred_element_type=F32)


def sigmoid(x):
    return 0.5 * jnp.tanh(0.5 * x) + 0.5


def layer_kernel(
    degree,
    chunk,
    idx_ref,
    ct_ref,
    mask_ref,
    own_ref,
    rim_ref,
    w_src_ref,
    w_half_ref,
    w_dst_ref,
    w_back_ref,
    w_cent_ref,
    gain_ref,
    ebias_ref,
    w_self_ref,
    w_agg_ref,
    nbias_ref,
    w_out_ref,
    updated_ref,
    down_ref,
    halo_ref,
    gw_ref,
    gv_ref,
    table,
    hid,
    slope,
    yhat,
    rstd,
    dmsg,
    dhid,
    ysums,
    dycs,
    bases,
    sums,
    hid_new,
    slope_new,
    dps,
    pds,
    cents,
    pres,
    dinners,
    sbs,
    dobs,
    live_ref,
    *accs,
):
    nodes, width = down_ref.shape
    listed = nodes + rim_ref.shape[0]
    copies = len(accs)
    steps = nodes // chunk
    edges = degree * chunk
    half = edges // 2
    groups = edges // 8

    table[pl.ds(0, nodes), :] = mm(own_ref[...], w_half_ref[...])
    table[pl.ds(nodes, listed - nodes), :] = mm(rim_ref[...], w_half_ref[...])
    table[pl.ds(listed, 8), :] = jnp.full((8, width), EMPTY, F32)
    for ref in (
        slope, yhat, rstd, dmsg, dhid, ysums, dycs, sums, hid, hid_new, slope_new, dps,
        cents, pres, dinners, sbs, dobs, *accs,
    ):
        ref[...] = jnp.zeros_like(ref)
    gw_ref[...] = jnp.zeros_like(gw_ref)

    ones = jnp.full((width, width), 1.0 / width, BF)
    zeros = jnp.zeros((width, width), BF)
    ones2 = jnp.concatenate(
        [jnp.concatenate([ones, zeros], 1), jnp.concatenate([zeros, ones], 1)], 0
    )
    lanes = mask_ref.shape[1]
    eye = lax.broadcasted_iota(jnp.int32, (lanes, lanes), 0) == (
        lax.broadcasted_iota(jnp.int32, (lanes, lanes), 1)
    )
    every = jnp.ones((lanes, width), BF)
    for g in range(nodes // lanes):
        row = mask_ref[g : g + 1, :].astype(F32)
        spread = jnp.where(eye, jnp.broadcast_to(row, (lanes, lanes)), 0.0)
        live_ref[pl.ds(g * lanes, lanes), :] = mm(spread.astype(BF), every).astype(BF)
    at_row = lax.broadcasted_iota(jnp.int32, (8, width), 0)
    bit = [(at_row & b) != 0 for b in (1, 2, 4)]
    only = [at_row == j for j in range(8)]

    def rows_of(m):
        return pl.ds(pl.multiple_of(jnp.clip(m, 0, steps - 1) * chunk, chunk), chunk)

    def list_of(m):
        at = jnp.clip(m, 0, steps - 1)
        return lambda e: idx_ref.at[pl.ds(e * steps, steps)][at]

    def body(m, carry):
        gain = gain_ref[...]

        def slot(lag, ring=RING):
            return lax.rem(m + 2 * ring - lag, ring)

        v = {"pd": pds[...]}
        per = chunk // 8
        dpd = [None] * per
        idx0 = list_of(m)
        idx7 = list_of(m - 7)
        s7 = slot(7)

        def wide(x):
            return jnp.concatenate([x[:half], x[half:]], 1)

        def fold(x):
            return sum(x[i * 8 : i * 8 + 8] for i in range(1, per)) + x[:8]

        def gather(g):
            rows = [
                jnp.broadcast_to(table[pl.ds(idx0(g * 8 + j), 1), :], (8, width))
                for j in range(8)
            ]
            for b in bit:
                rows = [jnp.where(b, q, p) for p, q in zip(rows[::2], rows[1::2])]
            n = g % per
            z = rows[0] + v["pd"][n * 8 : n * 8 + 8]
            t = jnp.tanh(z)
            q = 1.0 + t
            h = z * q
            slope_new[pl.ds(g * 8, 8), :] = q + h * (1.0 - t)
            return h

        def scatter(chunks):
            for g in chunks:
                at = pl.ds(g * 8, 8)
                dx = dhid[at, :] * slope[s7, at, :]
                n = g % per
                dpd[n] = dx if dpd[n] is None else dpd[n] + dx
                for j in range(8):
                    acc = accs[(g * 8 + j) % copies]
                    to = pl.ds(idx7(g * 8 + j) + (8 - j), 8)
                    pltpu.store(acc.at[to, :], acc[to, :] + dx, mask=only[j])

        def c1():
            old = hid_new[...]
            hid[slot(1)] = old
            slope[slot(1)] = slope_new[...]
            v["c"] = mm(wide(old), w_cent_ref[...])

        def c1s():
            cents[...] = v["c"]

        def c2():
            v["c2"] = cents[...]
            v["var"] = mm((v["c2"] * v["c2"]).astype(BF), ones2)

        def c3():
            r = lax.rsqrt(v["var"] + 1e-5)
            y = v["c2"] * r
            yhat[slot(2, 4)] = y
            rstd[slot(2, 4)] = r
            ys = y[:, :width] + y[:, width:]
            ysums[slot(2)] = (
                sum(ys[i * chunk : (i + 1) * chunk] for i in range(1, degree // 2))
                + ys[:chunk]
            )

        def n1():
            at = rows_of(m - 3)
            own = own_ref[at, :]
            sb = (ysums[slot(3)] * gain).astype(BF)
            v["pre"] = (
                mm(own, w_self_ref[...]) + mm(sb, w_agg_ref[...]) + nbias_ref[...]
            )
            inside = jnp.logical_and(m >= 3, m < steps + 3).astype(F32)
            dob = (inside * live_ref[at, :].astype(F32) * ct_ref[at, :]).astype(BF)
            v["dinner"] = mm_nt(dob, w_out_ref[...])
            v["sb"] = sb
            v["dob"] = dob

        def n1s():
            pres[...] = v["pre"]
            dinners[...] = v["dinner"]
            sbs[...] = v["sb"]
            dobs[...] = v["dob"]

        def n2():
            pre = pres[...]
            sg = sigmoid(pre)
            u = pre * sg
            v["ub"] = u.astype(BF)
            v["dpre"] = dinners[...] * (sg + u - u * sg)
            v["dpb"] = v["dpre"].astype(BF)
            v["dsum"] = mm_nt(v["dpb"], w_agg_ref[...])

        def n3():
            at = rows_of(m - 4)
            own = own_ref[at, :]
            updated_ref[at, :] = (
                own.astype(F32)
                + live_ref[at, :].astype(F32) * mm(v["ub"], w_out_ref[...])
            ).astype(BF)
            bases[slot(4, 5)] = ct_ref[at, :] + mm_nt(v["dpb"], w_self_ref[...])
            sums[2] += fold(v["dpre"])

        def n4():
            gw_ref[3] += mm_tn(own_ref[rows_of(m - 4), :], v["dpb"])
            gw_ref[4] += mm_tn(sbs[...], v["dpb"])
            gw_ref[5] += mm_tn(v["ub"], dobs[...])

        def n5():
            dy = v["dsum"] * gain
            dycs[...] = dy - jnp.mean(dy, axis=1, keepdims=True)
            sums[0] += fold(v["dsum"] * ysums[slot(4)])

        def d1():
            d = dycs[...]
            d = jnp.concatenate([d] * (degree // 2), 0)
            v["d"] = jnp.concatenate([d, d], 1)
            v["t"] = mm((v["d"] * yhat[slot(5, 4)]).astype(BF), ones2)

        def d2():
            y = yhat[slot(5, 4)]
            dm = (rstd[slot(5, 4)] * (v["d"] - y * v["t"])).astype(BF)
            dmsg[pl.ds(0, half), :] = dm[:, :width]
            dmsg[pl.ds(half, half), :] = dm[:, width:]

        def e1():
            v["dm"] = dmsg[...]
            v["dh"] = mm(wide(v["dm"]), w_back_ref[...])

        def e2():
            gw_ref[2] += mm_tn(hid[slot(6)], v["dm"])

        def e3(first, last):
            for g in range(first, last):
                if g * 8 < half:
                    part = v["dh"][g * 8 : g * 8 + 8, :width]
                else:
                    part = v["dh"][g * 8 - half : g * 8 - half + 8, width:]
                dhid[pl.ds(g * 8, 8), :] = part

        def f1():
            at = rows_of(m - 8)
            dp = dps[...]
            dpdb = dp.astype(BF)
            down_ref[at, :] = bases[slot(8, 5)] + mm_nt(dpdb, w_dst_ref[...])
            gw_ref[1] += mm_tn(own_ref[at, :], dpdb)
            sums[1] += fold(dp)

        def p1():
            own = own_ref[rows_of(m + 1), :]
            pds[...] = 0.5 * (mm(own, w_dst_ref[...]) + ebias_ref[...])

        stages = dict(
            c1=c1, c1s=c1s, c2=c2, c3=c3, n1=n1, n1s=n1s, n2=n2, n3=n3, n4=n4, n5=n5,
            d1=d1, d2=d2, e1=e1, e2=e2, f1=f1, p1=p1,
        )
        done = written = taken = 0
        for item in PLAN:
            if item == "e3":
                e3(written, done)
                written = done
            elif isinstance(item, str):
                stages[item]()
            else:
                kind, last = item[0], groups * item[1] // 24
                if kind == "s":
                    scatter(range(done, last))
                    done = last
                else:
                    for g in range(taken, last, 2):
                        pair = jnp.concatenate([gather(g), gather(g + 1)], 0)
                        hid_new[pl.ds(g * 8, 16), :] = pair.astype(BF)
                    taken = last
        e3(written, groups)
        dps[...] = jnp.concatenate(dpd, 0)
        return carry

    pds[...] = 0.5 * (mm(own_ref[pl.ds(0, chunk), :], w_dst_ref[...]) + ebias_ref[...])
    lax.fori_loop(0, steps + 8, body, 0)

    gv_ref[...] = jnp.concatenate(
        [jnp.sum(sums[i], axis=0, keepdims=True) for i in range(3)]
        + [jnp.zeros((5, width), F32)],
        0,
    )
    dproj = accs[0][pl.ds(8, listed), :]
    for acc in accs[1:]:
        dproj = dproj + acc[pl.ds(8, listed), :]
    dpb = dproj.astype(BF)
    dext = mm_nt(dpb, w_src_ref[...])
    down_ref[...] += dext[:nodes]
    halo_ref[...] = dext[nodes:].astype(BF)
    gw_ref[0] = mm_tn(own_ref[...], dpb[:nodes]) + mm_tn(rim_ref[...], dpb[nodes:])


def diagonal(w):
    zero = jnp.zeros_like(w)
    return jnp.concatenate(
        [jnp.concatenate([w, zero], 1), jnp.concatenate([zero, w], 1)], 0
    )


def layer(node_latent, rims, cotangent, neighbours, node_mask, weights):
    w_src, w_dst, w_msg, edge_gain, edge_bias, w_self, w_agg, node_bias, w_out = weights
    degree, nodes = neighbours.shape
    width = cotangent.shape[1]
    listed = nodes + rims.shape[0]
    chunk = min(CHUNK, nodes)
    steps = nodes // chunk
    edges = degree * chunk
    idx = jnp.where(neighbours < 0, listed, neighbours)
    idx = idx.reshape(degree, steps, chunk).transpose(0, 2, 1).reshape(-1)
    lanes = min(128, nodes)
    mask = node_mask.reshape(nodes // lanes, lanes)
    w32 = w_msg.astype(F32)
    w_cent = (w32 - jnp.mean(w32, axis=1, keepdims=True)).astype(BF)
    half = jnp.asarray(0.5, BF)
    vmem = pl.BlockSpec(memory_space=pltpu.VMEM)
    return pl.pallas_call(
        functools.partial(layer_kernel, degree, chunk),
        in_specs=[pl.BlockSpec(memory_space=pltpu.SMEM)] + [vmem] * 15,
        out_specs=[vmem] * 5,
        out_shape=[
            jax.ShapeDtypeStruct((nodes, width), BF),
            jax.ShapeDtypeStruct((nodes, width), F32),
            jax.ShapeDtypeStruct((listed - nodes, width), BF),
            jax.ShapeDtypeStruct((6, width, width), F32),
            jax.ShapeDtypeStruct((8, width), F32),
        ],
        scratch_shapes=[
            pltpu.VMEM((listed + 8, width), F32),
            pltpu.VMEM((RING, edges, width), BF),
            pltpu.VMEM((RING, edges, width), F32),
            pltpu.VMEM((4, edges // 2, 2 * width), F32),
            pltpu.VMEM((4, edges // 2, 2 * width), F32),
            pltpu.VMEM((edges, width), BF),
            pltpu.VMEM((edges, width), F32),
            pltpu.VMEM((RING, chunk, width), F32),
            pltpu.VMEM((chunk, width), F32),
            pltpu.VMEM((5, chunk, width), F32),
            pltpu.VMEM((3, 8, width), F32),
            pltpu.VMEM((edges, width), BF),
            pltpu.VMEM((edges, width), F32),
            pltpu.VMEM((chunk, width), F32),
            pltpu.VMEM((chunk, width), F32),
            pltpu.VMEM((edges // 2, 2 * width), F32),
            pltpu.VMEM((chunk, width), F32),
            pltpu.VMEM((chunk, width), F32),
            pltpu.VMEM((chunk, width), BF),
            pltpu.VMEM((chunk, width), BF),
            pltpu.VMEM((nodes, width), BF),
        ]
        + [pltpu.VMEM((listed + 24, width), F32)] * COPIES,
        compiler_params=pltpu.CompilerParams(vmem_limit_bytes=60 * 2**20),
        name="layer",
    )(
        idx,
        cotangent,
        mask,
        node_latent,
        rims,
        w_src,
        w_src * half,
        w_dst,
        diagonal(w_msg.T * half),
        diagonal(w_cent),
        edge_gain[None],
        edge_bias[None],
        w_self,
        w_agg,
        node_bias[None],
        w_out,
    )


def exchange_kernel(size, list_ref, own_ref, out_ref, own32, outbound, send_sem, recv_sem):
    rim = out_ref.shape[0] // 2
    width = out_ref.shape[1]
    me = lax.axis_index("tile")
    below = lax.rem(me + size - 1, size)
    above = lax.rem(me + 1, size)
    barrier = pltpu.get_barrier_semaphore()
    for other in (below, above):
        pl.semaphore_signal(
            barrier, inc=1, device_id={"tile": other}, device_id_type=MESH
        )
    own32[...] = own_ref[...].astype(F32)
    at_row = lax.broadcasted_iota(jnp.int32, (8, width), 0)
    bit = [(at_row & b) != 0 for b in (1, 2, 4)]
    step = 64

    def rows_at(base):
        rows = [
            jnp.broadcast_to(own32[pl.ds(list_ref[base + j], 1), :], (8, width))
            for j in range(8)
        ]
        for b in bit:
            rows = [jnp.where(b, q, p) for p, q in zip(rows[::2], rows[1::2])]
        return rows[0]

    def gather(t, carry):
        base = pl.multiple_of(t * step, step)
        part = jnp.concatenate([rows_at(base + g * 8) for g in range(step // 8)], 0)
        outbound[pl.ds(base, step), :] = part.astype(BF)
        return carry

    def send(here, there, other, sem):
        return pltpu.make_async_remote_copy(
            src_ref=outbound.at[pl.ds(here, rim)],
            dst_ref=out_ref.at[pl.ds(there, rim)],
            send_sem=send_sem.at[sem],
            recv_sem=recv_sem.at[sem],
            device_id={"tile": other},
            device_id_type=MESH,
        )

    to_above = send(rim, 0, above, 0)
    to_below = send(0, rim, below, 1)
    lax.fori_loop(rim // step, 2 * rim // step, gather, 0)
    pl.semaphore_wait(barrier, 2)
    to_above.start()
    lax.fori_loop(0, rim // step, gather, 0)
    to_below.start()
    to_above.wait()
    to_below.wait()


def exchange(listing, node_latent, size):
    count, width = listing.shape[0], node_latent.shape[1]
    vmem = pl.BlockSpec(memory_space=pltpu.VMEM)
    return pl.pallas_call(
        functools.partial(exchange_kernel, size),
        in_specs=[pl.BlockSpec(memory_space=pltpu.SMEM), vmem],
        out_specs=vmem,
        out_shape=jax.ShapeDtypeStruct((count, width), BF),
        scratch_shapes=[
            pltpu.VMEM(node_latent.shape, F32),
            pltpu.VMEM((count, width), BF),
            pltpu.SemaphoreType.DMA((2,)),
            pltpu.SemaphoreType.DMA((2,)),
        ],
        compiler_params=pltpu.CompilerParams(
            collective_id=0, has_side_effects=True, vmem_limit_bytes=32 * 2**20
        ),
        name="exchange",
    )(listing, node_latent)


def finish_kernel(list_ref, back_ref, down_ref, out_ref):
    count = out_ref.shape[0]
    first = pl.program_id(0) * count
    span = list_ref.shape[1]
    here = lax.broadcasted_iota(jnp.int32, (count, span), 0) + first
    hit = jnp.where(here == list_ref[...], 1.0, 0.0).astype(BF)
    out_ref[...] = down_ref[...] + mm(hit, back_ref[...])


def finish(listing, back, down):
    nodes, width = down.shape
    count = min(512, nodes)
    rowed = pl.BlockSpec((count, width), lambda i: (i, 0))
    return pl.pallas_call(
        finish_kernel,
        grid=(nodes // count,),
        in_specs=[
            pl.BlockSpec((1, listing.shape[1]), lambda i: (0, 0)),
            pl.BlockSpec(back.shape, lambda i: (0, 0)),
            rowed,
        ],
        out_specs=rowed,
        out_shape=jax.ShapeDtypeStruct((nodes, width), F32),
        compiler_params=pltpu.CompilerParams(
            dimension_semantics=("arbitrary",), vmem_limit_bytes=60 * 2**20
        ),
        name="finish",
    )(listing, back, down)


def total_over(value, axis):
    size = lax.axis_size(axis)
    if size & (size - 1):
        return lax.psum(value, axis)
    bit = 1
    while bit < size:
        other = lax.ppermute(value, axis, [(i, i ^ bit) for i in range(size)])
        value = (value.astype(F32) + other.astype(F32)).astype(BF)
        bit *= 2
    return value


def on_device(node_latent, cotangent, neighbours, send_rows, node_mask, *weights):
    nodes = node_latent.shape[0]
    rim = send_rows.shape[2]
    size = lax.axis_size("tile")
    up = [(i, (i + 1) % size) for i in range(size)]
    down = [(j, i) for i, j in up]
    listing = send_rows.reshape(1, 2 * rim)
    rims = exchange(listing[0], node_latent, size)
    updated, down_grad, halo, gw, gv = layer(
        node_latent, rims, cotangent, neighbours, node_mask, weights
    )
    to_below = lax.ppermute(halo[:rim], "tile", down)
    to_above = lax.ppermute(halo[rim:], "tile", up)
    back = jnp.concatenate([to_above, to_below], axis=0)
    packed = jnp.concatenate([gw.reshape(-1, gw.shape[2]), gv], axis=0).astype(BF)
    packed = total_over(packed, "tile").astype(F32)
    latent_grad = finish(listing, back, down_grad)
    packed = packed * (nodes * size) ** (-0.5)
    width = gw.shape[2]
    mats = [packed[i * width : (i + 1) * width] for i in range(6)]
    vecs = [packed[6 * width + i] for i in range(3)]
    return (
        updated,
        latent_grad,
        mats[0],
        mats[1],
        mats[2],
        vecs[0],
        vecs[1],
        mats[3],
        mats[4],
        vecs[2],
        mats[5],
    )


def solution(mesh):
    rowed, shared = P(("scene", "tile"), None), P()
    in_specs = (
        rowed,
        rowed,
        P(None, ("scene", "tile")),
        P(("scene", "tile"), None, None),
        P(("scene", "tile")),
    ) + (shared,) * 9
    mat, vec = P("scene", None), P("scene")
    out_specs = (rowed, rowed, mat, mat, mat, vec, vec, mat, mat, vec, mat)
    return jax.shard_map(
        on_device, mesh=mesh, in_specs=in_specs, out_specs=out_specs, check_vma=False
    )
```

```python
import functools

import jax
import jax.numpy as jnp
from jax import lax
from jax.experimental import pallas as pl
from jax.experimental.pallas import tpu as pltpu
from jax.sharding import PartitionSpec as P

CHUNK = 32
RING = 8
HALVES = 2
COPIES = 8
EMPTY = -1e4
PLAN = (
    "c1", "c2", ("s", 1), ("g", 1), "d1", "e1", ("s", 2), ("g", 2), "n2", "n1", ("s", 3), ("g", 3), "f1", "p1", ("s", 4), ("g", 4), ("s", 5), ("g", 5), "c1s", ("s", 6), ("g", 6), ("s", 7), ("g", 7), "d2", ("s", 8), ("g", 8), "e2", ("s", 9), ("g", 9), "n3", ("s", 10), ("g", 10), "n4", ("s", 11), ("g", 11), "n1s", ("s", 12), ("g", 12), "n5", ("s", 13), ("g", 13), "c3", ("s", 14), ("g", 14), "e3", ("s", 15), ("g", 15), ("s", 16), ("g", 16), "e3", ("s", 17), ("g", 17), ("s", 18), ("g", 18), ("s", 19), ("g", 19), ("s", 20), ("g", 20), ("s", 21), ("g", 21), ("s", 22), ("g", 22), ("s", 23), ("g", 23), "e3", ("s", 24), ("g", 24),
)
BF = jnp.bfloat16
F32 = jnp.float32
MESH = pl.DeviceIdType.MESH


def mm(a, b):
    return jnp.dot(a, b, preferred_element_type=F32)


def mm_nt(a, b):
    return lax.dot_general(a, b, (((1,), (1,)), ((), ())), preferred_element_type=F32)


def mm_tn(a, b):
    return lax.dot_general(a, b, (((0,), (0,)), ((), ())), preferred_element_type=F32)


def sigmoid(x):
    return 0.5 * jnp.tanh(0.5 * x) + 0.5


def layer_kernel(
    degree,
    chunk,
    idx_ref,
    ct_ref,
    mask_ref,
    own_ref,
    rim_ref,
    w_src_ref,
    w_dst_ref,
    w_msg_ref,
    gain_ref,
    ebias_ref,
    w_self_ref,
    w_agg_ref,
    nbias_ref,
    w_out_ref,
    updated_ref,
    down_ref,
    halo_ref,
    gw_ref,
    gv_ref,
    table,
    hid,
    slope,
    yhat,
    rstd,
    dmsg,
    dhid,
    ysums,
    dycs,
    bases,
    sums,
    hid_new,
    slope_new,
    dps,
    pds,
    cents,
    pres,
    dinners,
    sbs,
    dobs,
    live_ref,
    w_cent_ref,
    w_back_ref,
    *accs,
):
    nodes, width = down_ref.shape
    listed = nodes + rim_ref.shape[0]
    copies = len(accs)
    steps = nodes // chunk
    edges = degree * chunk
    half = edges // 2
    groups = edges // 8

    w_half = (0.5 * w_src_ref[...].astype(F32)).astype(BF)
    table[pl.ds(8, nodes), :] = mm(own_ref[...], w_half)
    table[pl.ds(8 + nodes, listed - nodes), :] = mm(rim_ref[...], w_half)
    table[pl.ds(0, 8), :] = jnp.full((8, width), EMPTY, F32)
    w32 = w_msg_ref[...].astype(F32)
    cent = (w32 - jnp.mean(w32, axis=1, keepdims=True)).astype(BF)
    back = (0.5 * w32).T.astype(BF)
    for ref, w in ((w_cent_ref, cent), (w_back_ref, back)):
        ref[...] = jnp.zeros_like(ref)
        ref[pl.ds(0, width), pl.ds(0, width)] = w
        ref[pl.ds(width, width), pl.ds(width, width)] = w
    for ref in (
        slope, yhat, rstd, dmsg, dhid, ysums, dycs, sums, hid, hid_new, slope_new, dps,
        cents, pres, dinners, sbs, dobs, *accs,
    ):
        ref[...] = jnp.zeros_like(ref)
    gw_ref[...] = jnp.zeros_like(gw_ref)

    ones = jnp.full((width, width), 1.0 / width, BF)
    zeros = jnp.zeros((width, width), BF)
    ones2 = jnp.concatenate(
        [jnp.concatenate([ones, zeros], 1), jnp.concatenate([zeros, ones], 1)], 0
    )
    lanes = mask_ref.shape[1]
    eye = lax.broadcasted_iota(jnp.int32, (lanes, lanes), 0) == (
        lax.broadcasted_iota(jnp.int32, (lanes, lanes), 1)
    )
    every = jnp.ones((lanes, width), BF)
    for g in range(nodes // lanes):
        row = mask_ref[g : g + 1, :].astype(F32)
        spread = jnp.where(eye, jnp.broadcast_to(row, (lanes, lanes)), 0.0)
        live_ref[pl.ds(g * lanes, lanes), :] = mm(spread.astype(BF), every).astype(BF)
    at_row = lax.broadcasted_iota(jnp.int32, (8, width), 0)
    bit = [(at_row & b) != 0 for b in (1, 2, 4)]
    only = [at_row == j for j in range(8)]

    def rows_of(m):
        return pl.ds(pl.multiple_of(jnp.clip(m, 0, steps - 1) * chunk, chunk), chunk)

    def list_of(m):
        at = jnp.clip(m, 0, steps - 1) * chunk
        far = nodes - chunk + 1

        def one(e):
            start = e // chunk * nodes + e % chunk
            return idx_ref.at[pl.ds(start, far)][at]

        return one

    def body(m, carry):
        gain = gain_ref[...]

        def slot(lag, ring=RING):
            return lax.rem(m + 2 * ring - lag, ring)

        v = {"pd": pds[...]}
        per = chunk // 8
        dpd = [None] * per
        idx0 = list_of(m)
        idx7 = list_of(m - 7)
        s7 = slot(7)

        def wide(x):
            return jnp.concatenate([x[:half], x[half:]], 1)

        def fold(x):
            return sum(x[i * 8 : i * 8 + 8] for i in range(1, per)) + x[:8]

        def gather(g):
            rows = [
                jnp.broadcast_to(table[pl.ds(idx0(g * 8 + j) + 8, 1), :], (8, width))
                for j in range(8)
            ]
            for b in bit:
                rows = [jnp.where(b, q, p) for p, q in zip(rows[::2], rows[1::2])]
            n = g % per
            z = rows[0] + v["pd"][n * 8 : n * 8 + 8]
            t = jnp.tanh(z)
            q = 1.0 + t
            h = z * q
            slope_new[pl.ds(g * 8, 8), :] = q + h * (1.0 - t)
            return h

        def scatter(chunks):
            for g in chunks:
                at = pl.ds(g * 8, 8)
                dx = dhid[at, :] * slope[s7, at, :]
                n = g % per
                dpd[n] = dx if dpd[n] is None else dpd[n] + dx
                for j in range(8):
                    acc = accs[(g * 8 + j) % copies]
                    to = pl.ds(idx7(g * 8 + j) + (8 - j), 8)
                    pltpu.store(acc.at[to, :], acc[to, :] + dx, mask=only[j])

        def c1():
            old = hid_new[...]
            hid[slot(1)] = old
            slope[slot(1)] = slope_new[...]
            v["c"] = mm(wide(old), w_cent_ref[...])

        def c1s():
            cents[...] = v["c"]

        def c2():
            v["c2"] = cents[...]
            v["var"] = mm((v["c2"] * v["c2"]).astype(BF), ones2)

        def c3():
            r = lax.rsqrt(v["var"] + 1e-5)
            y = v["c2"] * r
            yhat[slot(2, 4)] = y
            rstd[slot(2, 4)] = r
            ys = y[:, :width] + y[:, width:]
            ysums[slot(2)] = (
                sum(ys[i * chunk : (i + 1) * chunk] for i in range(1, degree // 2))
                + ys[:chunk]
            )

        def n1():
            at = rows_of(m - 3)
            own = own_ref[at, :]
            sb = (ysums[slot(3)] * gain).astype(BF)
            v["pre"] = (
                mm(own, w_self_ref[...]) + mm(sb, w_agg_ref[...]) + nbias_ref[...]
            )
            inside = jnp.logical_and(m >= 3, m < steps + 3).astype(F32)
            dob = (inside * live_ref[at, :].astype(F32) * ct_ref[at, :]).astype(BF)
            v["dinner"] = mm_nt(dob, w_out_ref[...])
            v["sb"] = sb
            v["dob"] = dob

        def n1s():
            pres[...] = v["pre"]
            dinners[...] = v["dinner"]
            sbs[...] = v["sb"]
            dobs[...] = v["dob"]

        def n2():
            pre = pres[...]
            sg = sigmoid(pre)
            u = pre * sg
            v["ub"] = u.astype(BF)
            v["dpre"] = dinners[...] * (sg + u - u * sg)
            v["dpb"] = v["dpre"].astype(BF)
            v["dsum"] = mm_nt(v["dpb"], w_agg_ref[...])

        def n3():
            at = rows_of(m - 4)
            own = own_ref[at, :]
            updated_ref[at, :] = (
                own.astype(F32)
                + live_ref[at, :].astype(F32) * mm(v["ub"], w_out_ref[...])
            ).astype(BF)
            bases[slot(4, 5)] = ct_ref[at, :] + mm_nt(v["dpb"], w_self_ref[...])
            sums[2] += fold(v["dpre"])

        def n4():
            gw_ref[3] += mm_tn(own_ref[rows_of(m - 4), :], v["dpb"])
            gw_ref[4] += mm_tn(sbs[...], v["dpb"])
            gw_ref[5] += mm_tn(v["ub"], dobs[...])

        def n5():
            dy = v["dsum"] * gain
            dycs[...] = dy - jnp.mean(dy, axis=1, keepdims=True)
            sums[0] += fold(v["dsum"] * ysums[slot(4)])

        def d1():
            d = dycs[...]
            d = jnp.concatenate([d] * (degree // 2), 0)
            v["d"] = jnp.concatenate([d, d], 1)
            v["t"] = mm((v["d"] * yhat[slot(5, 4)]).astype(BF), ones2)

        def d2():
            y = yhat[slot(5, 4)]
            dm = (rstd[slot(5, 4)] * (v["d"] - y * v["t"])).astype(BF)
            dmsg[pl.ds(0, half), :] = dm[:, :width]
            dmsg[pl.ds(half, half), :] = dm[:, width:]

        def e1():
            v["dm"] = dmsg[...]
            v["dh"] = mm(wide(v["dm"]), w_back_ref[...])

        def e2():
            gw_ref[2] += mm_tn(hid[slot(6)], v["dm"])

        def e3(first, last):
            for g in range(first, last):
                if g * 8 < half:
                    part = v["dh"][g * 8 : g * 8 + 8, :width]
                else:
                    part = v["dh"][g * 8 - half : g * 8 - half + 8, width:]
                dhid[pl.ds(g * 8, 8), :] = part

        def f1():
            at = rows_of(m - 8)
            dp = dps[...]
            dpdb = dp.astype(BF)
            down_ref[at, :] = bases[slot(8, 5)] + mm_nt(dpdb, w_dst_ref[...])
            gw_ref[1] += mm_tn(own_ref[at, :], dpdb)
            sums[1] += fold(dp)

        def p1():
            own = own_ref[rows_of(m + 1), :]
            pds[...] = 0.5 * (mm(own, w_dst_ref[...]) + ebias_ref[...])

        stages = dict(
            c1=c1, c1s=c1s, c2=c2, c3=c3, n1=n1, n1s=n1s, n2=n2, n3=n3, n4=n4, n5=n5,
            d1=d1, d2=d2, e1=e1, e2=e2, f1=f1, p1=p1,
        )
        done = written = taken = 0
        for item in PLAN:
            if item == "e3":
                e3(written, done)
                written = done
            elif isinstance(item, str):
                stages[item]()
            else:
                kind, last = item[0], groups * item[1] // 24
                if kind == "s":
                    scatter(range(done, last))
                    done = last
                else:
                    for g in range(taken, last, 2):
                        pair = jnp.concatenate([gather(g), gather(g + 1)], 0)
                        hid_new[pl.ds(g * 8, 16), :] = pair.astype(BF)
                    taken = last
        e3(written, groups)
        dps[...] = jnp.concatenate(dpd, 0)
        return carry

    pds[...] = 0.5 * (mm(own_ref[pl.ds(0, chunk), :], w_dst_ref[...]) + ebias_ref[...])
    lax.fori_loop(0, steps + 8, body, 0)

    gv_ref[...] = jnp.concatenate(
        [jnp.sum(sums[i], axis=0, keepdims=True) for i in range(3)]
        + [jnp.zeros((5, width), F32)],
        0,
    )
    dproj = accs[0][pl.ds(8, listed), :]
    for acc in accs[1:]:
        dproj = dproj + acc[pl.ds(8, listed), :]
    dpb = dproj.astype(BF)
    dext = mm_nt(dpb, w_src_ref[...])
    down_ref[...] += dext[:nodes]
    halo_ref[...] = dext[nodes:].astype(BF)
    gw_ref[0] = mm_tn(own_ref[...], dpb[:nodes]) + mm_tn(rim_ref[...], dpb[nodes:])


def layer(node_latent, rims, cotangent, neighbours, node_mask, weights):
    w_src, w_dst, w_msg, edge_gain, edge_bias, w_self, w_agg, node_bias, w_out = weights
    degree, nodes = neighbours.shape
    width = cotangent.shape[1]
    listed = nodes + rims.shape[0]
    chunk = min(CHUNK, nodes)
    edges = degree * chunk
    lanes = min(128, nodes)
    mask = node_mask.reshape(nodes // lanes, lanes)
    vmem = pl.BlockSpec(memory_space=pltpu.VMEM)
    return pl.pallas_call(
        functools.partial(layer_kernel, degree, chunk),
        in_specs=[pl.BlockSpec(memory_space=pltpu.SMEM)] + [vmem] * 13,
        out_specs=[vmem] * 5,
        out_shape=[
            jax.ShapeDtypeStruct((nodes, width), BF),
            jax.ShapeDtypeStruct((nodes, width), F32),
            jax.ShapeDtypeStruct((listed - nodes, width), BF),
            jax.ShapeDtypeStruct((6, width, width), F32),
            jax.ShapeDtypeStruct((8, width), F32),
        ],
        scratch_shapes=[
            pltpu.VMEM((listed + 8, width), F32),
            pltpu.VMEM((RING, edges, width), BF),
            pltpu.VMEM((RING, edges, width), F32),
            pltpu.VMEM((4, edges // 2, 2 * width), F32),
            pltpu.VMEM((4, edges // 2, 2 * width), F32),
            pltpu.VMEM((edges, width), BF),
            pltpu.VMEM((edges, width), F32),
            pltpu.VMEM((RING, chunk, width), F32),
            pltpu.VMEM((chunk, width), F32),
            pltpu.VMEM((5, chunk, width), F32),
            pltpu.VMEM((3, 8, width), F32),
            pltpu.VMEM((edges, width), BF),
            pltpu.VMEM((edges, width), F32),
            pltpu.VMEM((chunk, width), F32),
            pltpu.VMEM((chunk, width), F32),
            pltpu.VMEM((edges // 2, 2 * width), F32),
            pltpu.VMEM((chunk, width), F32),
            pltpu.VMEM((chunk, width), F32),
            pltpu.VMEM((chunk, width), BF),
            pltpu.VMEM((chunk, width), BF),
            pltpu.VMEM((nodes, width), BF),
            pltpu.VMEM((2 * width, 2 * width), BF),
            pltpu.VMEM((2 * width, 2 * width), BF),
        ]
        + [pltpu.VMEM((listed + 24, width), F32)] * COPIES,
        compiler_params=pltpu.CompilerParams(vmem_limit_bytes=60 * 2**20),
        name="layer",
    )(
        neighbours.reshape(-1),
        cotangent,
        mask,
        node_latent,
        rims,
        w_src,
        w_dst,
        w_msg,
        edge_gain[None],
        edge_bias[None],
        w_self,
        w_agg,
        node_bias[None],
        w_out,
    )


def exchange_kernel(size, list_ref, own_ref, out_ref, own32, outbound, send_sem, recv_sem):
    rim = out_ref.shape[0] // 2
    width = out_ref.shape[1]
    me = lax.axis_index("tile")
    below = lax.rem(me + size - 1, size)
    above = lax.rem(me + 1, size)
    barrier = pltpu.get_barrier_semaphore()
    for other in (below, above):
        pl.semaphore_signal(
            barrier, inc=1, device_id={"tile": other}, device_id_type=MESH
        )
    own32[...] = own_ref[...].astype(F32)
    at_row = lax.broadcasted_iota(jnp.int32, (8, width), 0)
    bit = [(at_row & b) != 0 for b in (1, 2, 4)]
    step = 64

    def rows_at(base):
        rows = [
            jnp.broadcast_to(own32[pl.ds(list_ref[base + j], 1), :], (8, width))
            for j in range(8)
        ]
        for b in bit:
            rows = [jnp.where(b, q, p) for p, q in zip(rows[::2], rows[1::2])]
        return rows[0]

    def gather(t, carry):
        base = pl.multiple_of(t * step, step)
        part = jnp.concatenate([rows_at(base + g * 8) for g in range(step // 8)], 0)
        outbound[pl.ds(base, step), :] = part.astype(BF)
        return carry

    def send(here, there, other, sem):
        return pltpu.make_async_remote_copy(
            src_ref=outbound.at[pl.ds(here, rim)],
            dst_ref=out_ref.at[pl.ds(there, rim)],
            send_sem=send_sem.at[sem],
            recv_sem=recv_sem.at[sem],
            device_id={"tile": other},
            device_id_type=MESH,
        )

    to_above = send(rim, 0, above, 0)
    to_below = send(0, rim, below, 1)
    lax.fori_loop(rim // step, 2 * rim // step, gather, 0)
    pl.semaphore_wait(barrier, 2)
    to_above.start()
    lax.fori_loop(0, rim // step, gather, 0)
    to_below.start()
    to_above.wait()
    to_below.wait()


def exchange(listing, node_latent, size):
    count, width = listing.shape[0], node_latent.shape[1]
    vmem = pl.BlockSpec(memory_space=pltpu.VMEM)
    return pl.pallas_call(
        functools.partial(exchange_kernel, size),
        in_specs=[pl.BlockSpec(memory_space=pltpu.SMEM), vmem],
        out_specs=vmem,
        out_shape=jax.ShapeDtypeStruct((count, width), BF),
        scratch_shapes=[
            pltpu.VMEM(node_latent.shape, F32),
            pltpu.VMEM((count, width), BF),
            pltpu.SemaphoreType.DMA((2,)),
            pltpu.SemaphoreType.DMA((2,)),
        ],
        compiler_params=pltpu.CompilerParams(
            collective_id=0, has_side_effects=True, vmem_limit_bytes=32 * 2**20
        ),
        name="exchange",
    )(listing, node_latent)


def finish_kernel(
    size,
    scale,
    list_ref,
    halo_ref,
    down_ref,
    gw_ref,
    gv_ref,
    out_ref,
    total_ref,
    back,
    packed,
    parts,
    mine,
    gathered,
    halo_send,
    halo_recv,
    part_send,
    part_recv,
    full_send,
    full_recv,
):
    nodes, width = out_ref.shape
    rim = halo_ref.shape[0] // 2
    piece = mine.shape[0]
    me = lax.axis_index("tile")
    others = [lax.rem(me + d, size) for d in range(1, size)]
    barrier = pltpu.get_barrier_semaphore()
    for other in others:
        pl.semaphore_signal(
            barrier, inc=1, device_id={"tile": other}, device_id_type=MESH
        )

    def copy(src, dst, send, recv, other):
        return pltpu.make_async_remote_copy(
            src_ref=src,
            dst_ref=dst,
            send_sem=send,
            recv_sem=recv,
            device_id={"tile": other},
            device_id_type=MESH,
        )

    mats = gw_ref.shape[0] * width
    for i in range(gw_ref.shape[0]):
        packed[pl.ds(i * width, width), :] = gw_ref[i].astype(BF)
    rest = packed.shape[0] - mats
    packed[pl.ds(mats, rest), :] = jnp.concatenate(
        [gv_ref[...], jnp.zeros((rest - gv_ref.shape[0], width), F32)], 0
    ).astype(BF)

    def piece_of(ref, at):
        return ref.at[pl.ds(pl.multiple_of(at * piece, 16), piece)]

    spread = [
        copy(piece_of(packed, o), parts.at[d], part_send.at[d], part_recv.at[d], o)
        for d, o in enumerate(others)
    ]
    share = [
        copy(mine, piece_of(gathered, me), full_send.at[d], full_recv.at[d], o)
        for d, o in enumerate(others)
    ]
    span = rim // HALVES
    homes = []
    for i in range(HALVES):
        for here, there, other in ((rim, 0, others[0]), (0, rim, others[-1])):
            n = len(homes)
            homes.append(
                (
                    there + i * span,
                    copy(
                        halo_ref.at[pl.ds(here + i * span, span)],
                        back.at[pl.ds(there + i * span, span)],
                        halo_send.at[n],
                        halo_recv.at[n],
                        other,
                    ),
                )
            )

    pl.semaphore_wait(barrier, size - 1)
    for c in spread:
        c.start()
    for _, c in homes[:2]:
        c.start()
    out_ref[...] = down_ref[...]
    for c in spread:
        c.wait_recv()
    total = packed[pl.ds(pl.multiple_of(me * piece, 16), piece), :].astype(F32)
    for d in range(size - 1):
        total = total + parts[d].astype(F32)
    mine[...] = total.astype(BF)
    gathered[pl.ds(pl.multiple_of(me * piece, 16), piece), :] = total.astype(BF)
    for c in share:
        c.start()
    for _, c in homes[2:]:
        c.start()

    rows = min(512, nodes)
    for at, c in homes:
        c.wait_recv()

        def place(b, carry):
            first = pl.multiple_of(b * rows, rows)
            here = lax.broadcasted_iota(jnp.int32, (rows, span), 0) + first
            hit = jnp.where(here == list_ref[:, at : at + span], 1.0, 0.0).astype(BF)
            out_ref[pl.ds(first, rows), :] += mm(hit, back[pl.ds(at, span), :])
            return carry

        lax.fori_loop(0, nodes // rows, place, 0)

    for c in share:
        c.wait_recv()
    total_ref[...] = gathered[...].astype(F32) * scale
    for c in spread + share + [c for _, c in homes]:
        c.wait_send()


def finish(listing, halo, down, gw, gv, size, scale):
    nodes, width = down.shape
    need = gw.shape[0] * gw.shape[1] + gv.shape[0]
    piece = -(-need // (16 * size)) * 16
    vmem = pl.BlockSpec(memory_space=pltpu.VMEM)
    dma = pltpu.SemaphoreType.DMA
    return pl.pallas_call(
        functools.partial(finish_kernel, size, scale),
        in_specs=[vmem] * 5,
        out_specs=[vmem] * 2,
        out_shape=[
            jax.ShapeDtypeStruct((nodes, width), F32),
            jax.ShapeDtypeStruct((size * piece, width), F32),
        ],
        scratch_shapes=[
            pltpu.VMEM(halo.shape, BF),
            pltpu.VMEM((size * piece, width), BF),
            pltpu.VMEM((size - 1, piece, width), BF),
            pltpu.VMEM((piece, width), BF),
            pltpu.VMEM((size * piece, width), BF),
            dma((2 * HALVES,)),
            dma((2 * HALVES,)),
            dma((size - 1,)),
            dma((size - 1,)),
            dma((size - 1,)),
            dma((size - 1,)),
        ],
        compiler_params=pltpu.CompilerParams(
            collective_id=1, has_side_effects=True, vmem_limit_bytes=32 * 2**20
        ),
        name="finish",
    )(listing, halo, down, gw, gv)


def on_device(node_latent, cotangent, neighbours, send_rows, node_mask, *weights):
    nodes = node_latent.shape[0]
    size = lax.axis_size("tile")
    listing = send_rows.reshape(1, -1)
    rims = exchange(listing[0], node_latent, size)
    updated, down_grad, halo, gw, gv = layer(
        node_latent, rims, cotangent, neighbours, node_mask, weights
    )
    latent_grad, packed = finish(
        listing, halo, down_grad, gw, gv, size, (nodes * size) ** (-0.5)
    )
    width = gw.shape[2]
    mats = [packed[i * width : (i + 1) * width] for i in range(6)]
    vecs = [packed[6 * width + i] for i in range(3)]
    return (
        updated,
        latent_grad,
        mats[0],
        mats[1],
        mats[2],
        vecs[0],
        vecs[1],
        mats[3],
        mats[4],
        vecs[2],
        mats[5],
    )


def solution(mesh):
    rowed, shared = P(("scene", "tile"), None), P()
    in_specs = (
        rowed,
        rowed,
        P(None, ("scene", "tile")),
        P(("scene", "tile"), None, None),
        P(("scene", "tile")),
    ) + (shared,) * 9
    mat, vec = P("scene", None), P("scene")
    out_specs = (rowed, rowed, mat, mat, mat, vec, vec, mat, mat, vec, mat)
    return jax.shard_map(
        on_device, mesh=mesh, in_specs=in_specs, out_specs=out_specs, check_vma=False
    )
```

```python
import functools

import jax
import jax.numpy as jnp
from jax import lax
from jax.experimental import pallas as pl
from jax.experimental.pallas import tpu as pltpu
from jax.sharding import PartitionSpec as P

CHUNK = 32
RING = 8
HALVES = 2
COPIES = 8
EMPTY = -1e4
PLAN = (
    "c1", "c2", ("s", 1), ("g", 1), "d1", "e1", ("s", 2), ("g", 2), "n2", "n1", ("s", 3), ("g", 3), "f1", "p1", ("s", 4), ("g", 4), ("s", 5), ("g", 5), "c1s", ("s", 6), ("g", 6), ("s", 7), ("g", 7), "d2", ("s", 8), ("g", 8), "e2", ("s", 9), ("g", 9), "n3", ("s", 10), ("g", 10), "n4", ("s", 11), ("g", 11), "n1s", ("s", 12), ("g", 12), "n5", ("s", 13), ("g", 13), "c3", ("s", 14), ("g", 14), "e3", ("s", 15), ("g", 15), ("s", 16), ("g", 16), "e3", ("s", 17), ("g", 17), ("s", 18), ("g", 18), ("s", 19), ("g", 19), ("s", 20), ("g", 20), ("s", 21), ("g", 21), ("s", 22), ("g", 22), ("s", 23), ("g", 23), "e3", ("s", 24), ("g", 24),
)
BF = jnp.bfloat16
F32 = jnp.float32
MESH = pl.DeviceIdType.MESH


def mm(a, b):
    return jnp.dot(a, b, preferred_element_type=F32)


def mm_nt(a, b):
    return lax.dot_general(a, b, (((1,), (1,)), ((), ())), preferred_element_type=F32)


def mm_tn(a, b):
    return lax.dot_general(a, b, (((0,), (0,)), ((), ())), preferred_element_type=F32)


def sigmoid(x):
    return 0.5 * jnp.tanh(0.5 * x) + 0.5


def layer_kernel(
    degree,
    chunk,
    idx_hbm,
    ct_hbm,
    mask_ref,
    own_ref,
    rim_ref,
    w_src_ref,
    w_dst_ref,
    w_msg_ref,
    gain_ref,
    ebias_ref,
    w_self_ref,
    w_agg_ref,
    nbias_ref,
    w_out_ref,
    updated_hbm,
    down_ref,
    halo_ref,
    packed_ref,
    table,
    hid,
    slope,
    yhat,
    rstd,
    dmsg,
    dhid,
    ysums,
    dycs,
    bases,
    sums,
    hid_new,
    slope_new,
    dps,
    pds,
    cents,
    pres,
    dinners,
    sbs,
    dobs,
    live_ref,
    w_cent_ref,
    w_back_ref,
    gw_ref,
    idx_ref,
    ct_ref,
    updated_ref,
    local_sem,
    *accs,
):
    fetch_idx = pltpu.make_async_copy(idx_hbm, idx_ref, local_sem.at[0])
    fetch_ct = pltpu.make_async_copy(ct_hbm, ct_ref, local_sem.at[1])
    fetch_idx.start()
    fetch_ct.start()
    nodes, width = down_ref.shape
    listed = nodes + rim_ref.shape[0]
    copies = len(accs)
    steps = nodes // chunk
    edges = degree * chunk
    half = edges // 2
    groups = edges // 8

    w_half = (0.5 * w_src_ref[...].astype(F32)).astype(BF)
    table[pl.ds(8, nodes), :] = mm(own_ref[...], w_half)
    table[pl.ds(8 + nodes, listed - nodes), :] = mm(rim_ref[...], w_half)
    table[pl.ds(0, 8), :] = jnp.full((8, width), EMPTY, F32)
    w32 = w_msg_ref[...].astype(F32)
    cent = (w32 - jnp.mean(w32, axis=1, keepdims=True)).astype(BF)
    back = (0.5 * w32).T.astype(BF)
    for ref, w in ((w_cent_ref, cent), (w_back_ref, back)):
        ref[...] = jnp.zeros_like(ref)
        ref[pl.ds(0, width), pl.ds(0, width)] = w
        ref[pl.ds(width, width), pl.ds(width, width)] = w
    for ref in (
        slope, yhat, rstd, dmsg, dhid, ysums, dycs, sums, hid, hid_new, slope_new, dps,
        cents, pres, dinners, sbs, dobs, *accs,
    ):
        ref[...] = jnp.zeros_like(ref)
    gw_ref[...] = jnp.zeros_like(gw_ref)

    ones = jnp.full((width, width), 1.0 / width, BF)
    zeros = jnp.zeros((width, width), BF)
    ones2 = jnp.concatenate(
        [jnp.concatenate([ones, zeros], 1), jnp.concatenate([zeros, ones], 1)], 0
    )
    lanes = mask_ref.shape[1]
    eye = lax.broadcasted_iota(jnp.int32, (lanes, lanes), 0) == (
        lax.broadcasted_iota(jnp.int32, (lanes, lanes), 1)
    )
    every = jnp.ones((lanes, width), BF)
    for g in range(nodes // lanes):
        row = mask_ref[g : g + 1, :].astype(F32)
        spread = jnp.where(eye, jnp.broadcast_to(row, (lanes, lanes)), 0.0)
        live_ref[pl.ds(g * lanes, lanes), :] = mm(spread.astype(BF), every).astype(BF)
    at_row = lax.broadcasted_iota(jnp.int32, (8, width), 0)
    bit = [(at_row & b) != 0 for b in (1, 2, 4)]
    only = [at_row == j for j in range(8)]

    def rows_of(m):
        return pl.ds(pl.multiple_of(jnp.clip(m, 0, steps - 1) * chunk, chunk), chunk)

    def list_of(m):
        at = jnp.clip(m, 0, steps - 1) * chunk
        far = nodes - chunk + 1

        def one(e):
            start = e // chunk * nodes + e % chunk
            return idx_ref.at[pl.ds(start, far)][at]

        return one

    def body(m, carry):
        gain = gain_ref[...]

        def slot(lag, ring=RING):
            return lax.rem(m + 2 * ring - lag, ring)

        v = {"pd": pds[...]}
        per = chunk // 8
        dpd = [None] * per
        idx0 = list_of(m)
        idx7 = list_of(m - 7)
        s7 = slot(7)

        def wide(x):
            return jnp.concatenate([x[:half], x[half:]], 1)

        def fold(x):
            return sum(x[i * 8 : i * 8 + 8] for i in range(1, per)) + x[:8]

        def gather(g):
            rows = [
                jnp.broadcast_to(table[pl.ds(idx0(g * 8 + j) + 8, 1), :], (8, width))
                for j in range(8)
            ]
            for b in bit:
                rows = [jnp.where(b, q, p) for p, q in zip(rows[::2], rows[1::2])]
            n = g % per
            z = rows[0] + v["pd"][n * 8 : n * 8 + 8]
            t = jnp.tanh(z)
            q = 1.0 + t
            h = z * q
            slope_new[pl.ds(g * 8, 8), :] = q + h * (1.0 - t)
            return h

        def scatter(chunks):
            for g in chunks:
                at = pl.ds(g * 8, 8)
                dx = dhid[at, :] * slope[s7, at, :]
                n = g % per
                dpd[n] = dx if dpd[n] is None else dpd[n] + dx
                for j in range(8):
                    acc = accs[(g * 8 + j) % copies]
                    to = pl.ds(idx7(g * 8 + j) + (8 - j), 8)
                    pltpu.store(acc.at[to, :], acc[to, :] + dx, mask=only[j])

        def c1():
            old = hid_new[...]
            hid[slot(1)] = old
            slope[slot(1)] = slope_new[...]
            v["c"] = mm(wide(old), w_cent_ref[...])

        def c1s():
            cents[...] = v["c"]

        def c2():
            v["c2"] = cents[...]
            v["var"] = mm((v["c2"] * v["c2"]).astype(BF), ones2)

        def c3():
            r = lax.rsqrt(v["var"] + 1e-5)
            y = v["c2"] * r
            yhat[slot(2, 4)] = y
            rstd[slot(2, 4)] = r
            ys = y[:, :width] + y[:, width:]
            ysums[slot(2)] = (
                sum(ys[i * chunk : (i + 1) * chunk] for i in range(1, degree // 2))
                + ys[:chunk]
            )

        def n1():
            at = rows_of(m - 3)
            own = own_ref[at, :]
            sb = (ysums[slot(3)] * gain).astype(BF)
            v["pre"] = (
                mm(own, w_self_ref[...]) + mm(sb, w_agg_ref[...]) + nbias_ref[...]
            )
            inside = jnp.logical_and(m >= 3, m < steps + 3).astype(F32)
            dob = (inside * live_ref[at, :].astype(F32) * ct_ref[at, :]).astype(BF)
            v["dinner"] = mm_nt(dob, w_out_ref[...])
            v["sb"] = sb
            v["dob"] = dob

        def n1s():
            pres[...] = v["pre"]
            dinners[...] = v["dinner"]
            sbs[...] = v["sb"]
            dobs[...] = v["dob"]

        def n2():
            pre = pres[...]
            sg = sigmoid(pre)
            u = pre * sg
            v["ub"] = u.astype(BF)
            v["dpre"] = dinners[...] * (sg + u - u * sg)
            v["dpb"] = v["dpre"].astype(BF)
            v["dsum"] = mm_nt(v["dpb"], w_agg_ref[...])

        def n3():
            at = rows_of(m - 4)
            own = own_ref[at, :]
            updated_ref[at, :] = (
                own.astype(F32)
                + live_ref[at, :].astype(F32) * mm(v["ub"], w_out_ref[...])
            ).astype(BF)
            bases[slot(4, 5)] = ct_ref[at, :] + mm_nt(v["dpb"], w_self_ref[...])
            sums[2] += fold(v["dpre"])

        def n4():
            gw_ref[3] += mm_tn(own_ref[rows_of(m - 4), :], v["dpb"])
            gw_ref[4] += mm_tn(sbs[...], v["dpb"])
            gw_ref[5] += mm_tn(v["ub"], dobs[...])

        def n5():
            dy = v["dsum"] * gain
            dycs[...] = dy - jnp.mean(dy, axis=1, keepdims=True)
            sums[0] += fold(v["dsum"] * ysums[slot(4)])

        def d1():
            d = dycs[...]
            d = jnp.concatenate([d] * (degree // 2), 0)
            v["d"] = jnp.concatenate([d, d], 1)
            v["t"] = mm((v["d"] * yhat[slot(5, 4)]).astype(BF), ones2)

        def d2():
            y = yhat[slot(5, 4)]
            dm = (rstd[slot(5, 4)] * (v["d"] - y * v["t"])).astype(BF)
            dmsg[pl.ds(0, half), :] = dm[:, :width]
            dmsg[pl.ds(half, half), :] = dm[:, width:]

        def e1():
            v["dm"] = dmsg[...]
            v["dh"] = mm(wide(v["dm"]), w_back_ref[...])

        def e2():
            gw_ref[2] += mm_tn(hid[slot(6)], v["dm"])

        def e3(first, last):
            for g in range(first, last):
                if g * 8 < half:
                    part = v["dh"][g * 8 : g * 8 + 8, :width]
                else:
                    part = v["dh"][g * 8 - half : g * 8 - half + 8, width:]
                dhid[pl.ds(g * 8, 8), :] = part

        def f1():
            at = rows_of(m - 8)
            dp = dps[...]
            dpdb = dp.astype(BF)
            down_ref[at, :] = bases[slot(8, 5)] + mm_nt(dpdb, w_dst_ref[...])
            gw_ref[1] += mm_tn(own_ref[at, :], dpdb)
            sums[1] += fold(dp)

        def p1():
            own = own_ref[rows_of(m + 1), :]
            pds[...] = 0.5 * (mm(own, w_dst_ref[...]) + ebias_ref[...])

        stages = dict(
            c1=c1, c1s=c1s, c2=c2, c3=c3, n1=n1, n1s=n1s, n2=n2, n3=n3, n4=n4, n5=n5,
            d1=d1, d2=d2, e1=e1, e2=e2, f1=f1, p1=p1,
        )
        done = written = taken = 0
        for item in PLAN:
            if item == "e3":
                e3(written, done)
                written = done
            elif isinstance(item, str):
                stages[item]()
            else:
                kind, last = item[0], groups * item[1] // 24
                if kind == "s":
                    scatter(range(done, last))
                    done = last
                else:
                    for g in range(taken, last, 2):
                        pair = jnp.concatenate([gather(g), gather(g + 1)], 0)
                        hid_new[pl.ds(g * 8, 16), :] = pair.astype(BF)
                    taken = last
        e3(written, groups)
        dps[...] = jnp.concatenate(dpd, 0)
        return carry

    pds[...] = 0.5 * (mm(own_ref[pl.ds(0, chunk), :], w_dst_ref[...]) + ebias_ref[...])
    fetch_idx.wait()
    fetch_ct.wait()
    lax.fori_loop(0, steps + 8, body, 0)
    put_updated = pltpu.make_async_copy(updated_ref, updated_hbm, local_sem.at[2])
    put_updated.start()

    dproj = accs[0][pl.ds(8, listed), :]
    for acc in accs[1:]:
        dproj = dproj + acc[pl.ds(8, listed), :]
    dpb = dproj.astype(BF)
    dext = mm_nt(dpb, w_src_ref[...])
    down_ref[...] += dext[:nodes]
    halo_ref[...] = dext[nodes:].astype(BF)
    gw_ref[0] = mm_tn(own_ref[...], dpb[:nodes]) + mm_tn(rim_ref[...], dpb[nodes:])
    for i in range(gw_ref.shape[0]):
        packed_ref[pl.ds(i * width, width), :] = gw_ref[i].astype(BF)
    mats = gw_ref.shape[0] * width
    packed_ref[pl.ds(mats, packed_ref.shape[0] - mats), :] = jnp.concatenate(
        [jnp.sum(sums[i], axis=0, keepdims=True) for i in range(3)]
        + [jnp.zeros((packed_ref.shape[0] - mats - 3, width), F32)],
        0,
    ).astype(BF)
    put_updated.wait()


def layer(node_latent, rims, cotangent, neighbours, node_mask, weights, packed):
    w_src, w_dst, w_msg, edge_gain, edge_bias, w_self, w_agg, node_bias, w_out = weights
    degree, nodes = neighbours.shape
    width = cotangent.shape[1]
    listed = nodes + rims.shape[0]
    chunk = min(CHUNK, nodes)
    edges = degree * chunk
    lanes = min(128, nodes)
    mask = node_mask.reshape(nodes // lanes, lanes)
    vmem = pl.BlockSpec(memory_space=pltpu.VMEM)
    hbm = pl.BlockSpec(memory_space=pl.ANY)
    return pl.pallas_call(
        functools.partial(layer_kernel, degree, chunk),
        in_specs=[hbm, hbm] + [vmem] * 12,
        out_specs=[hbm] + [vmem] * 3,
        out_shape=[
            jax.ShapeDtypeStruct((nodes, width), BF),
            jax.ShapeDtypeStruct((nodes, width), F32),
            jax.ShapeDtypeStruct((listed - nodes, width), BF),
            jax.ShapeDtypeStruct((packed, width), BF),
        ],
        scratch_shapes=[
            pltpu.VMEM((listed + 8, width), F32),
            pltpu.VMEM((RING, edges, width), BF),
            pltpu.VMEM((RING, edges, width), F32),
            pltpu.VMEM((4, edges // 2, 2 * width), F32),
            pltpu.VMEM((4, edges // 2, 2 * width), F32),
            pltpu.VMEM((edges, width), BF),
            pltpu.VMEM((edges, width), F32),
            pltpu.VMEM((RING, chunk, width), F32),
            pltpu.VMEM((chunk, width), F32),
            pltpu.VMEM((5, chunk, width), F32),
            pltpu.VMEM((3, 8, width), F32),
            pltpu.VMEM((edges, width), BF),
            pltpu.VMEM((edges, width), F32),
            pltpu.VMEM((chunk, width), F32),
            pltpu.VMEM((chunk, width), F32),
            pltpu.VMEM((edges // 2, 2 * width), F32),
            pltpu.VMEM((chunk, width), F32),
            pltpu.VMEM((chunk, width), F32),
            pltpu.VMEM((chunk, width), BF),
            pltpu.VMEM((chunk, width), BF),
            pltpu.VMEM((nodes, width), BF),
            pltpu.VMEM((2 * width, 2 * width), BF),
            pltpu.VMEM((2 * width, 2 * width), BF),
            pltpu.VMEM((6, width, width), F32),
            pltpu.SMEM((degree * nodes,), jnp.int32),
            pltpu.VMEM((nodes, width), F32),
            pltpu.VMEM((nodes, width), BF),
            pltpu.SemaphoreType.DMA((3,)),
        ]
        + [pltpu.VMEM((listed + 24, width), F32)] * COPIES,
        compiler_params=pltpu.CompilerParams(vmem_limit_bytes=60 * 2**20),
        name="layer",
    )(
        neighbours.reshape(-1),
        cotangent,
        mask,
        node_latent,
        rims,
        w_src,
        w_dst,
        w_msg,
        edge_gain[None],
        edge_bias[None],
        w_self,
        w_agg,
        node_bias[None],
        w_out,
    )


def exchange_kernel(
    size, list_ref, own_ref, out_ref, own16, own32, outbound, send_sem, recv_sem, local_sem
):
    fetch = pltpu.make_async_copy(own_ref, own16, local_sem)
    fetch.start()
    rim = out_ref.shape[0] // 2
    width = out_ref.shape[1]
    me = lax.axis_index("tile")
    below = lax.rem(me + size - 1, size)
    above = lax.rem(me + 1, size)
    barrier = pltpu.get_barrier_semaphore()
    for other in (below, above):
        pl.semaphore_signal(
            barrier, inc=1, device_id={"tile": other}, device_id_type=MESH
        )
    fetch.wait()
    own32[...] = own16[...].astype(F32)
    at_row = lax.broadcasted_iota(jnp.int32, (8, width), 0)
    bit = [(at_row & b) != 0 for b in (1, 2, 4)]
    step = 64

    def rows_at(base):
        rows = [
            jnp.broadcast_to(own32[pl.ds(list_ref[base + j], 1), :], (8, width))
            for j in range(8)
        ]
        for b in bit:
            rows = [jnp.where(b, q, p) for p, q in zip(rows[::2], rows[1::2])]
        return rows[0]

    def gather(t, carry):
        base = pl.multiple_of(t * step, step)
        part = jnp.concatenate([rows_at(base + g * 8) for g in range(step // 8)], 0)
        outbound[pl.ds(base, step), :] = part.astype(BF)
        return carry

    span = rim // HALVES
    sent = []
    for i in range(HALVES):
        for here, there, other in ((rim, 0, above), (0, rim, below)):
            n = len(sent)
            start = here + i * span
            lax.fori_loop(start // step, (start + span) // step, gather, 0)
            if n == 0:
                pl.semaphore_wait(barrier, 2)
            c = pltpu.make_async_remote_copy(
                src_ref=outbound.at[pl.ds(start, span)],
                dst_ref=out_ref.at[pl.ds(there + i * span, span)],
                send_sem=send_sem.at[n],
                recv_sem=recv_sem.at[n],
                device_id={"tile": other},
                device_id_type=MESH,
            )
            c.start()
            sent.append(c)
    for c in sent:
        c.wait()


def exchange(listing, node_latent, size):
    count, width = listing.shape[0], node_latent.shape[1]
    vmem = pl.BlockSpec(memory_space=pltpu.VMEM)
    return pl.pallas_call(
        functools.partial(exchange_kernel, size),
        in_specs=[
            pl.BlockSpec(memory_space=pltpu.SMEM),
            pl.BlockSpec(memory_space=pl.ANY),
        ],
        out_specs=vmem,
        out_shape=jax.ShapeDtypeStruct((count, width), BF),
        scratch_shapes=[
            pltpu.VMEM(node_latent.shape, BF),
            pltpu.VMEM(node_latent.shape, F32),
            pltpu.VMEM((count, width), BF),
            pltpu.SemaphoreType.DMA((2 * HALVES,)),
            pltpu.SemaphoreType.DMA((2 * HALVES,)),
            pltpu.SemaphoreType.DMA,
        ],
        compiler_params=pltpu.CompilerParams(
            collective_id=0, has_side_effects=True, vmem_limit_bytes=60 * 2**20
        ),
        name="exchange",
    )(listing, node_latent)


def finish_kernel(
    size,
    scale,
    list_ref,
    halo_ref,
    down_ref,
    packed,
    out_ref,
    total_ref,
    back,
    halo,
    parts,
    mine,
    gathered,
    halo_send,
    halo_recv,
    part_send,
    part_recv,
    full_send,
    full_recv,
    local_sem,
):
    nodes, width = out_ref.shape
    rim = halo_ref.shape[0] // 2
    fetch_halo = pltpu.make_async_copy(halo_ref, halo, local_sem.at[0])
    fetch_down = pltpu.make_async_copy(down_ref, out_ref, local_sem.at[1])
    fetch_halo.start()
    fetch_down.start()
    piece = mine.shape[0]
    me = lax.axis_index("tile")
    others = [lax.rem(me + d, size) for d in range(1, size)]
    barrier = pltpu.get_barrier_semaphore()
    for other in others:
        pl.semaphore_signal(
            barrier, inc=1, device_id={"tile": other}, device_id_type=MESH
        )

    def copy(src, dst, send, recv, other):
        return pltpu.make_async_remote_copy(
            src_ref=src,
            dst_ref=dst,
            send_sem=send,
            recv_sem=recv,
            device_id={"tile": other},
            device_id_type=MESH,
        )

    def piece_of(ref, at):
        return ref.at[pl.ds(pl.multiple_of(at * piece, 16), piece)]

    spread = [
        copy(piece_of(packed, o), parts.at[d], part_send.at[d], part_recv.at[d], o)
        for d, o in enumerate(others)
    ]
    share = [
        copy(mine, piece_of(gathered, me), full_send.at[d], full_recv.at[d], o)
        for d, o in enumerate(others)
    ]
    span = rim // HALVES
    homes = []
    for i in range(HALVES):
        for here, there, other in ((rim, 0, others[0]), (0, rim, others[-1])):
            n = len(homes)
            homes.append(
                (
                    there + i * span,
                    copy(
                        halo.at[pl.ds(here + i * span, span)],
                        back.at[pl.ds(there + i * span, span)],
                        halo_send.at[n],
                        halo_recv.at[n],
                        other,
                    ),
                )
            )

    pl.semaphore_wait(barrier, size - 1)
    for c in spread:
        c.start()
    fetch_halo.wait()
    for _, c in homes[:2]:
        c.start()
    for c in spread:
        c.wait_recv()
    total = packed[pl.ds(pl.multiple_of(me * piece, 16), piece), :].astype(F32)
    for d in range(size - 1):
        total = total + parts[d].astype(F32)
    mine[...] = total.astype(BF)
    gathered[pl.ds(pl.multiple_of(me * piece, 16), piece), :] = total.astype(BF)
    for c in share:
        c.start()
    for _, c in homes[2:]:
        c.start()

    fetch_down.wait()
    rows = min(512, nodes)
    for at, c in homes:
        c.wait_recv()

        def place(b, carry):
            first = pl.multiple_of(b * rows, rows)
            here = lax.broadcasted_iota(jnp.int32, (rows, span), 0) + first
            hit = jnp.where(here == list_ref[:, at : at + span], 1.0, 0.0).astype(BF)
            out_ref[pl.ds(first, rows), :] += mm(hit, back[pl.ds(at, span), :])
            return carry

        lax.fori_loop(0, nodes // rows, place, 0)

    for c in share:
        c.wait_recv()
    total_ref[...] = gathered[...].astype(F32) * scale
    for c in spread + share + [c for _, c in homes]:
        c.wait_send()


def finish(listing, halo, down, packed, size, scale):
    nodes, width = down.shape
    piece = packed.shape[0] // size
    vmem = pl.BlockSpec(memory_space=pltpu.VMEM)
    hbm = pl.BlockSpec(memory_space=pl.ANY)
    dma = pltpu.SemaphoreType.DMA
    return pl.pallas_call(
        functools.partial(finish_kernel, size, scale),
        in_specs=[vmem, hbm, hbm, vmem],
        out_specs=[vmem] * 2,
        out_shape=[
            jax.ShapeDtypeStruct((nodes, width), F32),
            jax.ShapeDtypeStruct((size * piece, width), F32),
        ],
        scratch_shapes=[
            pltpu.VMEM(halo.shape, BF),
            pltpu.VMEM(halo.shape, BF),
            pltpu.VMEM((size - 1, piece, width), BF),
            pltpu.VMEM((piece, width), BF),
            pltpu.VMEM((size * piece, width), BF),
            dma((2 * HALVES,)),
            dma((2 * HALVES,)),
            dma((size - 1,)),
            dma((size - 1,)),
            dma((size - 1,)),
            dma((size - 1,)),
            dma((2,)),
        ],
        compiler_params=pltpu.CompilerParams(
            collective_id=1, has_side_effects=True, vmem_limit_bytes=60 * 2**20
        ),
        name="finish",
    )(listing, halo, down, packed)


def on_device(node_latent, cotangent, neighbours, send_rows, node_mask, *weights):
    nodes = node_latent.shape[0]
    size = lax.axis_size("tile")
    listing = send_rows.reshape(1, -1)
    rims = exchange(listing[0], node_latent, size)
    width = node_latent.shape[1]
    need = 6 * width + 3
    piece = -(-need // (16 * size)) * 16
    updated, down_grad, halo, packed = layer(
        node_latent, rims, cotangent, neighbours, node_mask, weights, size * piece
    )
    latent_grad, packed = finish(
        listing, halo, down_grad, packed, size, (nodes * size) ** (-0.5)
    )
    mats = [packed[i * width : (i + 1) * width] for i in range(6)]
    vecs = [packed[6 * width + i] for i in range(3)]
    return (
        updated,
        latent_grad,
        mats[0],
        mats[1],
        mats[2],
        vecs[0],
        vecs[1],
        mats[3],
        mats[4],
        vecs[2],
        mats[5],
    )


def solution(mesh):
    rowed, shared = P(("scene", "tile"), None), P()
    in_specs = (
        rowed,
        rowed,
        P(None, ("scene", "tile")),
        P(("scene", "tile"), None, None),
        P(("scene", "tile")),
    ) + (shared,) * 9
    mat, vec = P("scene", None), P("scene")
    out_specs = (rowed, rowed, mat, mat, mat, vec, vec, mat, mat, vec, mat)
    return jax.shard_map(
        on_device, mesh=mesh, in_specs=in_specs, out_specs=out_specs, check_vma=False
    )
```
